512 devices in a mesh: half: 2 (over x_lo), gx: 16 (over y, core), gy: 16 (over z, x_hi).
Axes of the slice: x: 4 (x_hi: 2, x_lo: 2; x = x_hi * 2 + x_lo), y: 8, z: 8, core: 2. Of those that a mesh axis runs over, the one named last changes fastest.
Arguments:
- current: float32 [2, 128, 73728], P('half', 'gx', 'gy'), may hold values from -6 to 6
- previous: float32 [2, 128, 73728], P('half', 'gx', 'gy'), may hold values from -6 to 6
- material: float32 [2, 128, 73728], P('half', 'gx', 'gy'), may hold values from 0.4 to 1.6
- prior: float32 [4, 128, 512], P(None, 'gx', 'gy'), may hold values from -6 to 6
Outputs:
- fields: float32 [2, 128, 73728], P('half', 'gx', 'gy')
- seafloor: float32 [2, 4, 128, 512], P('half', None, 'gx', 'gy')
The draws below stay inside these ranges and needn't reach their ends.
All inputs are finite; a program needn't handle non-finite values.
Results may differ from the reference program's by a relative error of at most 0.00002.
Values sent between devices are 32-bit elements; how exact they have to be, the bound alone decides.
A program may use at most 64 MiB of HBM per device.

```python
import math
import jax
import jax.numpy as jnp

STEPS = 4
PLANES = 144
NX = 128
NY = 512


def level_of(rng, dims, split, low, largest):
    factor_of, own = 1.0, jax.random.fold_in(rng, 6)
    for axis_at, shards_of in split:
        heights = jnp.exp(jax.random.uniform(jax.random.fold_in(own, axis_at), (shards_of,), jnp.float32, low / len(split), largest / len(split)))
        factor_of = factor_of * jnp.repeat(heights, dims[axis_at] // shards_of).reshape([-1 if axis == axis_at else 1 for axis in range(len(dims))])
    return factor_of


def gaussian(stream_key, shape, spread, limit, split=(), kind=jnp.bfloat16):
    result = jax.random.normal(stream_key, shape, jnp.float32) * spread
    if len(split) > 0:
        result = level_of(stream_key, shape, split, -0.22, 0.18) * result
    return jnp.clip(result, min=-limit, max=limit).astype(kind)


def setup_inputs(seed: int = 0) -> dict:
    splits = jax.random.split(jax.random.key(seed), 5)
    return {
        "current": gaussian(splits[0], (2, NX, NY * PLANES), 1.0, 6.0, ((0, 2), (1, 16), (2, 16)), jnp.float32),
        "previous": gaussian(splits[1], (2, NX, NY * PLANES), 1.0, 6.0, ((0, 2), (1, 16), (2, 16)), jnp.float32),
        "material": jnp.clip(jnp.exp(math.log(1.6) - 1.3862944 * jax.random.uniform(splits[2], (2, NX, NY * PLANES), jnp.float32) ** level_of(splits[2], (2, NX, NY * PLANES), ((0, 2), (1, 16), (2, 16)), -0.2, 0.2)), 0.4, 1.6),
        "prior": gaussian(splits[3], (STEPS, NX, NY), 1.0, 6.0, ((1, 16), (2, 16)), jnp.float32),
    }


TIME_STEP = 0.22
RELAXATION = 0.5


def water_march(pressure, earlier, speed_sq, forcing):
    samples = []
    for instant in range(STEPS):
        samples.append(pressure[:, :, -1])
        ghost_row = pressure[:, :, -1:] - forcing[instant][:, :, None]
        column = jnp.concatenate([jnp.zeros_like(ghost_row), pressure, ghost_row], axis=2)
        padded = jnp.pad(column, ((1, 1), (1, 1), (0, 0)))
        laplace = (padded[2:, 1:-1, 1:-1] + padded[:-2, 1:-1, 1:-1] + padded[1:-1, 2:, 1:-1]
                   + padded[1:-1, :-2, 1:-1] + padded[1:-1, 1:-1, 2:] + padded[1:-1, 1:-1, :-2]
                   - 6.0 * pressure)
        pressure, earlier = 2.0 * pressure - earlier + TIME_STEP * TIME_STEP * speed_sq * laplace, pressure
    return pressure, jnp.stack(samples)


def derivatives(padded):
    centre = padded[1:-1, 1:-1, 1:-1]
    curve_xx = padded[2:, 1:-1, 1:-1] - 2.0 * centre + padded[:-2, 1:-1, 1:-1]
    curve_yy = padded[1:-1, 2:, 1:-1] - 2.0 * centre + padded[1:-1, :-2, 1:-1]
    curve_zz = padded[1:-1, 1:-1, 2:] - 2.0 * centre + padded[1:-1, 1:-1, :-2]
    cross_xy = (padded[2:, 2:, 1:-1] - padded[2:, :-2, 1:-1] - padded[:-2, 2:, 1:-1] + padded[:-2, :-2, 1:-1]) * 0.25
    cross_xz = (padded[2:, 1:-1, 2:] - padded[2:, 1:-1, :-2] - padded[:-2, 1:-1, 2:] + padded[:-2, 1:-1, :-2]) * 0.25
    cross_yz = (padded[1:-1, 2:, 2:] - padded[1:-1, 2:, :-2] - padded[1:-1, :-2, 2:] + padded[1:-1, :-2, :-2]) * 0.25
    return curve_xx, curve_yy, curve_zz, cross_xy, cross_xz, cross_yz


def seabed_march(displace, earlier, moduli, samples):
    thick = displace.shape[2] // 3
    bulk_mod = moduli[:, :, :thick]
    shear_mod = moduli[:, :, thick:2 * thick]
    buoyancy = moduli[:, :, 2 * thick:]
    surface = (jnp.arange(thick) == 0).astype(displace.dtype)
    motions = []
    for instant in range(STEPS):
        pieces = [derivatives(jnp.pad(displace[:, :, component * thick:(component + 1) * thick], 1))
                  for component in range(3)]
        grad_x = pieces[0][0] + pieces[1][3] + pieces[2][4]
        grad_y = pieces[0][3] + pieces[1][1] + pieces[2][5]
        grad_z = pieces[0][4] + pieces[1][5] + pieces[2][2]
        accels = []
        for component, grad_term in enumerate((grad_x, grad_y, grad_z)):
            laplace = pieces[component][0] + pieces[component][1] + pieces[component][2]
            accels.append(buoyancy * (bulk_mod * grad_term + shear_mod * laplace))
        accels[2] = accels[2] + buoyancy * surface * samples[instant][:, :, None]
        motions.append(accels[2][:, :, 0])
        stacked = jnp.concatenate(accels, axis=2)
        displace, earlier = 2.0 * displace - earlier + TIME_STEP * TIME_STEP * stacked, displace
    return displace, jnp.stack(motions)


def reference(current, previous, material, prior):
    cube = (2, NX, NY, PLANES)
    current = current.reshape(cube)
    previous = previous.reshape(cube)
    material = material.reshape(cube)
    water, trace = water_march(current[0], previous[0], material[0], prior)
    seabed, motion = seabed_march(current[1], previous[1], material[1], trace)
    fields = jnp.stack([water, seabed]).reshape((2, NX, NY * PLANES))
    seafloor = jnp.stack([RELAXATION * motion + (1.0 - RELAXATION) * prior, trace])
    return fields, seafloor
```

```python
import functools

import jax
import jax.numpy as jnp
from jax import lax
from jax.experimental import pallas as pl
from jax.experimental.pallas import tpu as pltpu
from jax.sharding import PartitionSpec as P

STEPS = 4
PLANES = 144
THICK = PLANES // 3
TIME_STEP = 0.22
RELAXATION = 0.5
H2 = TIME_STEP * TIME_STEP

LANES = 128
ROWS = 16
PAD = 8
PERIOD = 9
MESH = pl.DeviceIdType.MESH
DIRS = tuple((dx, dy) for dx in (-1, 0, 1) for dy in (-1, 0, 1) if (dx, dy) != (0, 0))


def lanes_of(tile, count=1):
    start = (tile + PAD) * LANES
    if not isinstance(start, int):
        start = pl.multiple_of(start, LANES)
    return pl.ds(start, count * LANES)


def rows_sent(dx):
    return {0: pl.ds(0, 8), 1: pl.ds(4, 4), -1: pl.ds(0, 4)}[dx]


def rows_landed(dx):
    return {0: pl.ds(0, 8), 1: pl.ds(12, 4), -1: pl.ds(8, 4)}[dx]


def shift_x(value, by):
    return pltpu.roll(value, (-by) % ROWS, 0)


def turn(value, by):
    return pltpu.roll(value, (-by) % LANES, 1)


class Tiles:
    def __init__(self):
        self.known = {}

    def get(self, name, tile, make):
        key = (name, tile)
        if key not in self.known:
            self.known[key] = make()
        return self.known[key]


def flat_shift(memo, name, of, lane, tile, by):
    whole, part = divmod(by, LANES)
    first = memo.get(("turn", name, part), tile + whole, lambda: turn(of(tile + whole), part))
    if part == 0:
        return first
    second = memo.get(("turn", name, part), tile + whole + 1, lambda: turn(of(tile + whole + 1), part))
    return jnp.where(lane < LANES - part, first, second)


def seabed_block(src, old, dst, ca, cb, mod, kinds, zlow, zhigh, load, dst_pad, base, tiles, last):
    memo = Tiles()
    lane = lax.broadcasted_iota(jnp.int32, (ROWS, LANES), 1)
    rows = 8 if last else ROWS
    lane_out = lane[:rows]

    def at(ref, j):
        return ref[:, lanes_of(base + j)]

    def pattern(ref, j):
        return memo.get(id(ref), j % PERIOD, lambda: ref[:, pl.ds((j % PERIOD) * LANES, LANES)])

    def u(j):
        return memo.get("u", j, lambda: at(src, j))

    def zp(j):
        return memo.get("zp", j, lambda: flat_shift(memo, "u", u, lane, j, 1) * pattern(zhigh, j))

    def zm(j):
        return memo.get("zm", j, lambda: flat_shift(memo, "u", u, lane, j, -1) * pattern(zlow, j))

    def yp(j):
        return memo.get("yp", j, lambda: flat_shift(memo, "u", u, lane, j, PLANES))

    def ym(j):
        return memo.get("ym", j, lambda: flat_shift(memo, "u", u, lane, j, -PLANES))

    def slope_z(j):
        return memo.get("sz", j, lambda: zp(j) - zm(j))

    def slope_y(j):
        return memo.get("sy", j, lambda: yp(j) - ym(j))

    def cross_x(value):
        return (shift_x(value, 1) - shift_x(value, -1))[:rows]

    def cross_xy(j):
        return memo.get("xy", j, lambda: cross_x(slope_y(j)))

    def cross_xz(j):
        return memo.get("xz", j, lambda: cross_x(slope_z(j)))

    def slope_z_out(j):
        return memo.get("szo", j, lambda: slope_z(j)[:rows])

    def cross_yz(j):
        return memo.get(
            "yz", j,
            lambda: flat_shift(memo, "szo", slope_z_out, lane_out, j, PLANES)
            - flat_shift(memo, "szo", slope_z_out, lane_out, j, -PLANES),
        )

    def kind(j):
        return pattern(kinds, j)[:rows]

    def toward_low(j):
        return memo.get("w1", j, lambda: jnp.where(kind(j) == 1, cross_xy(j), cross_yz(j)))

    def toward_high(j):
        return memo.get("w2", j, lambda: jnp.where(kind(j) == 0, cross_xy(j), cross_yz(j)))

    out = {}
    for j in tiles:
        first, third = kind(j) == 0, kind(j) == 2
        from_high = flat_shift(memo, "w1", toward_low, lane_out, j, THICK)
        from_low = flat_shift(memo, "w2", toward_high, lane_out, j, -THICK)
        far_high = flat_shift(memo, "xz", cross_xz, lane_out, j, 2 * THICK)
        far_low = flat_shift(memo, "xz", cross_xz, lane_out, j, -2 * THICK)
        mixed = jnp.where(third, far_low, from_high) + jnp.where(first, far_high, from_low)
        lap_x = (shift_x(u(j), 1) + shift_x(u(j), -1))[:rows]
        lap_y = (yp(j) + ym(j))[:rows]
        lap_z = (zp(j) + zm(j))[:rows]
        centre = u(j)[:rows]
        twice = centre + centre
        own = jnp.where(first, lap_x, jnp.where(third, lap_z, lap_y)) - twice
        lap = lap_x + lap_y + lap_z - 6.0 * centre
        acc = at(ca, j)[:rows] * (own + 0.25 * mixed) + at(cb, j)[:rows] * lap
        pushed = load(j)
        if pushed is not None:
            acc = acc + (H2 * at(mod, j)[:rows]) * pushed[:rows]
        new = twice - at(old, j)[:rows] + acc
        if last:
            dst[:, pl.ds(dst_pad + j * LANES, LANES)] = new
        else:
            dst[:, lanes_of(base + j)] = new
        out[j] = acc
    return out


def water_block(src, old, dst, mod, ghost, dst_pad, base, tiles, last):
    memo = Tiles()
    lane = lax.broadcasted_iota(jnp.int32, (ROWS, LANES), 1)
    rows = 8 if last else ROWS

    def at(ref, j):
        return ref[:, lanes_of(base + j)]

    def u(j):
        return memo.get("u", j, lambda: at(src, j))

    for j in tiles:
        below = flat_shift(memo, "u", u, lane, j, 1)
        above = flat_shift(memo, "u", u, lane, j, -1)
        offset = (j * LANES) % PLANES
        top = (-offset) % PLANES
        floor = PLANES - 1 - offset
        if top < LANES:
            above = jnp.where(lane == top, 0.0, above)
        if 0 <= floor < LANES:
            below = jnp.where(lane == floor, u(j) - ghost(j), below)
        total = (shift_x(u(j), 1) + shift_x(u(j), -1)) + (below + above)
        total = total + (flat_shift(memo, "u", u, lane, j, PLANES) + flat_shift(memo, "u", u, lane, j, -PLANES))
        total = (total - 6.0 * u(j))[:rows]
        centre = u(j)[:rows]
        new = (centre + centre) - at(old, j)[:rows] + (H2 * at(mod, j)[:rows]) * total
        if last:
            dst[:, pl.ds(dst_pad + j * LANES, LANES)] = new
        else:
            dst[:, lanes_of(base + j)] = new


def floor_lane(tile):
    if tile % PERIOD == 0:
        return None
    return (tile - 1) // PERIOD, 16 * ((tile - 1) % PERIOD) + 15


def top_lane(tile):
    place = {0: 0, 1: 1, 3: 2, 4: 3, 5: 4, 6: 5, 7: 6, 8: 7}.get(tile % PERIOD)
    if place is None:
        return None
    return tile // PERIOD, (16 * place + 2 * THICK) % LANES


def exact_dot(a, b):
    return jnp.dot(a, b, precision=lax.Precision.HIGHEST, preferred_element_type=jnp.float32)


def kernel(
    sizes, own_tiles, cur_hbm, prev_hbm, mat_hbm, prior_hbm, fields_ref, floor_ref,
    cur, prev, mat, p1, p2, p3, ca, cb, kinds, zlow, zhigh, prior, rims, packed, arrived, spread, columns, moved, returned,
    load_sem, send_sem, recv_sem, prior_send, prior_recv, trace_send, trace_recv, move_send, move_recv,
):
    half, gx, gy = lax.axis_index("half"), lax.axis_index("gx"), lax.axis_index("gy")
    n_x, n_y = sizes
    wet = half == 0
    groups = own_tiles // PERIOD

    def exists(dx, dy):
        x, y = gx + dx, gy + dy
        return (x >= 0) & (x < n_x) & (y >= 0) & (y < n_y)

    loads = [
        pltpu.make_async_copy(src.at[0], dst.at[0:8, lanes_of(0, own_tiles)], load_sem.at[n])
        for n, (src, dst) in enumerate(((cur_hbm, cur), (prev_hbm, prev), (mat_hbm, mat)))
    ]
    loads.append(pltpu.make_async_copy(prior_hbm, prior, load_sem.at[3]))
    for copy in loads:
        copy.start()

    barrier = pltpu.get_barrier_semaphore()
    count = jnp.int32(1)
    for dx, dy in DIRS:
        here = exists(dx, dy)
        count = count + here.astype(jnp.int32)

        @pl.when(here)
        def _(dx=dx, dy=dy):
            pl.semaphore_signal(barrier, inc=1, device_id={"gx": gx + dx, "gy": gy + dy}, device_id_type=MESH)

    pl.semaphore_signal(barrier, inc=1, device_id={"half": 1 - half}, device_id_type=MESH)

    flat = lax.broadcasted_iota(jnp.int32, (ROWS, PERIOD * LANES), 1)
    plane = flat % PLANES
    part = plane // THICK
    level = plane - part * THICK
    kinds[...] = part
    zlow[...] = (level != 0).astype(jnp.float32)
    zhigh[...] = (level != THICK - 1).astype(jnp.float32)

    def halo_copies(dx, dy):
        out = []
        for n, (ref, width) in enumerate(((cur, 5), (prev, 4), (mat, 4))):
            if dy == 0:
                src_lanes = dst_lanes = lanes_of(0, own_tiles)
            elif dy == 1:
                src_lanes, dst_lanes = lanes_of(own_tiles - width, width), lanes_of(-width, width)
            else:
                src_lanes, dst_lanes = lanes_of(0, width), lanes_of(own_tiles, width)
            slot = DIRS.index((dx, dy)) * 3 + n
            out.append(
                pltpu.make_async_remote_copy(
                    src_ref=ref.at[rows_sent(dx), src_lanes],
                    dst_ref=ref.at[rows_landed(dx), dst_lanes],
                    send_sem=send_sem.at[slot],
                    recv_sem=recv_sem.at[slot],
                    device_id={"gx": gx + dx, "gy": gy + dy},
                    device_id_type=MESH,
                )
            )
        return out

    def prior_copy(dx, dy):
        slot = DIRS.index((dx, dy))
        return pltpu.make_async_remote_copy(
            src_ref=prior.at[pl.ds(0, STEPS - 1)],
            dst_ref=rims.at[slot],
            send_sem=prior_send.at[slot],
            recv_sem=prior_recv.at[slot],
            device_id={"gx": gx + dx, "gy": gy + dy},
            device_id_type=MESH,
        )

    blank = jnp.zeros((ROWS, LANES), jnp.float32)
    for ref, reach in ((mat, 5), (p1, 5), (p2, 4), (p3, 3)):
        ref[:, lanes_of(-reach)] = blank
        ref[:, lanes_of(own_tiles + reach - 1)] = blank

    for dx, dy in DIRS:
        @pl.when(jnp.logical_not(exists(-dx, -dy)))
        def _(dx=dx, dy=dy):
            lanes = {0: lanes_of(0, own_tiles), 1: lanes_of(-5, 5), -1: lanes_of(own_tiles, 5)}[dy]
            for ref in (cur, prev, mat):
                ref[rows_landed(dx), lanes] = jnp.zeros((8 if dx == 0 else 4, lanes.size), jnp.float32)
            rims[DIRS.index((dx, dy))] = jnp.zeros(rims.shape[1:], jnp.float32)

    for copy in loads:
        copy.wait()
    pl.semaphore_wait(barrier, count)

    order = sorted(DIRS, key=lambda d: (d[1] == 0, d[0] != 0))
    for dx, dy in order:
        @pl.when(exists(dx, dy))
        def _(dx=dx, dy=dy):
            for copy in halo_copies(dx, dy):
                copy.start()

            @pl.when(wet)
            def _():
                prior_copy(dx, dy).start()

    for dx, dy in DIRS:
        @pl.when(exists(-dx, -dy))
        def _(dx=dx, dy=dy):
            for copy in halo_copies(dx, dy):
                copy.wait_recv()

            @pl.when(wet)
            def _():
                prior_copy(dx, dy).wait_recv()

    lane = lax.broadcasted_iota(jnp.int32, (ROWS, LANES), 1)
    levels = (cur, p1, p2, p3)
    olds = (prev, cur, p1, p2)
    width = own_tiles * LANES

    def over_tiles(block, t):
        margin = STEPS - 1 - t
        edge = -(-margin * PLANES // LANES)
        if edge:
            block(0, range(-edge, 0), 0)
        @pl.loop(0, groups)
        def _(g):
            block(g * PERIOD, range(PERIOD), g + 1)

        if edge:
            block(own_tiles, range(edge), groups + 1)

    def trace_copy(t):
        return pltpu.make_async_remote_copy(
            src_ref=packed.at[t], dst_ref=arrived.at[t], send_sem=trace_send.at[t], recv_sem=trace_recv.at[t],
            device_id={"half": 1 - half}, device_id_type=MESH,
        )

    def move_copy(t):
        return pltpu.make_async_remote_copy(
            src_ref=moved.at[t], dst_ref=returned.at[t], send_sem=move_send.at[t], recv_sem=move_recv.at[t],
            device_id={"half": 1 - half}, device_id_type=MESH,
        )

    def dense(value, first):
        cells = 8 * groups
        row = lax.broadcasted_iota(jnp.int32, (LANES, cells), 0)
        col = lax.broadcasted_iota(jnp.int32, (LANES, cells), 1)
        pick = (row == 16 * (col % 8) + first + col // 8).astype(jnp.float32)
        return exact_dot(value, pick)

    @pl.when(wet)
    def _():
        cells = 8 * groups
        row = lax.broadcasted_iota(jnp.int32, (cells, groups * LANES), 0)
        col = lax.broadcasted_iota(jnp.int32, (cells, groups * LANES), 1)
        place = (col == LANES * (row // 8) + 16 * (row % 8) + 15).astype(jnp.float32)
        upper = lax.broadcasted_iota(jnp.int32, (8, cells), 0) < 4

        def rim(dx, dy, t):
            return rims[DIRS.index((dx, dy)), t]

        for t in range(STEPS):
            centre = prior[t]
            if t == STEPS - 1:
                spread[t, 0:8, pl.ds(LANES, groups * LANES)] = exact_dot(centre, place)
                continue
            for dy, value in (
                (0, jnp.concatenate([centre, jnp.where(upper, rim(-1, 0, t), rim(1, 0, t))], 0)),
                (1, jnp.concatenate([rim(0, 1, t), jnp.where(upper, rim(-1, 1, t), rim(1, 1, t))], 0)),
                (-1, jnp.concatenate([rim(0, -1, t), jnp.where(upper, rim(-1, -1, t), rim(1, -1, t))], 0)),
            ):
                if dy == 0:
                    spread[t, :, pl.ds(LANES, groups * LANES)] = exact_dot(value, place)
                elif dy == 1:
                    spread[t, :, pl.ds(0, LANES)] = exact_dot(value, place[:, (groups - 1) * LANES:])
                else:
                    spread[t, :, pl.ds((groups + 1) * LANES, LANES)] = exact_dot(value, place[:, :LANES])

        for t in range(STEPS):
            src, old = levels[t], olds[t]
            margin = STEPS - 1 - t
            total = None
            for g in range(-1, groups + 1):
                tile = None
                for j in range(8):
                    q = g * PERIOD + j + 1
                    edge = -(-margin * PLANES // LANES)
                    if q < -edge or q >= own_tiles + edge:
                        continue
                    value = src[:, lanes_of(q)]
                    tile = value if tile is None else jnp.where(lane == 16 * j + 15, value, tile)
                if tile is None:
                    continue
                tile = jnp.where(lane % 16 == 15, tile, 0.0)
                tile = turn(tile, 15 - (g + 1))
                total = tile if total is None else total + tile
            packed[t] = total
            trace_copy(t).start()

            def block(base, tiles, slot, t=t, src=src, old=old):
                last = t == STEPS - 1
                start = 0
                if last:
                    start = pl.multiple_of(base * LANES, LANES)

                def ghost(j):
                    at = slot * LANES
                    if not isinstance(at, int):
                        at = pl.multiple_of(at, LANES)
                    return spread[t, :, pl.ds(at, LANES)]

                dst = fields_ref.at[0] if last else levels[t + 1]
                water_block(src, old, dst, mat, ghost, start, base, tiles, last)

            over_tiles(block, t)

        for t in range(STEPS):
            move_copy(t).wait_recv()
            floor_ref[0, t] = RELAXATION * dense(returned[t], 0) + (1.0 - RELAXATION) * prior[t]
            trace_copy(t).wait_send()

    @pl.when(jnp.logical_not(wet))
    def _():
        def moduli(base, tiles, slot):
            memo = Tiles()

            def m(j):
                return memo.get("m", j, lambda: mat[:, lanes_of(base + j)])

            for j in tiles:
                which = kinds[:, pl.ds((j % PERIOD) * LANES, LANES)]
                first, third = which == 0, which == 2
                up1 = flat_shift(memo, "m", m, lane, j, THICK)
                up2 = flat_shift(memo, "m", m, lane, j, 2 * THICK)
                down1 = flat_shift(memo, "m", m, lane, j, -THICK)
                down2 = flat_shift(memo, "m", m, lane, j, -2 * THICK)
                bulk = jnp.where(first, m(j), jnp.where(third, down2, down1))
                shear = jnp.where(first, up1, jnp.where(third, down1, m(j)))
                light = H2 * jnp.where(first, up2, jnp.where(third, m(j), up1))
                ca[:, lanes_of(base + j)] = light * bulk
                cb[:, lanes_of(base + j)] = light * shear

        over_tiles(moduli, 0)

        for t in range(STEPS):
            src, old = levels[t], olds[t]
            last = t == STEPS - 1
            trace_copy(t).wait_recv()
            for g in range(-1, groups + 1):
                spread[t, :, pl.ds((g + 1) * LANES, LANES)] = turn(arrived[t], (g + 1) - 2 * THICK)

            def block(base, tiles, slot, t=t, src=src, old=old, last=last):
                start = pl.multiple_of(base * LANES, LANES) if last else 0

                def load(j):
                    spot = top_lane(j)
                    if spot is None:
                        return None
                    at = slot * LANES
                    if not isinstance(at, int):
                        at = pl.multiple_of(at, LANES)
                    value = spread[t, :, pl.ds(at, LANES)]
                    return jnp.where(lane == spot[1], value, 0.0)

                dst = fields_ref.at[0] if last else levels[t + 1]
                acc = seabed_block(
                    src, old, dst, ca, cb, mat, kinds, zlow, zhigh, load, start, base, tiles, last
                )
                if len(tiles) == PERIOD:
                    tile = None
                    for j in tiles:
                        spot = top_lane(j)
                        if spot is not None:
                            value = acc[j][:8]
                            tile = value if tile is None else jnp.where(lane[:8] == spot[1], value, tile)
                    at = pl.multiple_of((slot - 1) * LANES, LANES)
                    columns[:, pl.ds(at, LANES)] = tile

            over_tiles(block, t)
            total = None
            for g in range(groups):
                tile = columns[:, pl.ds(g * LANES, LANES)] * (1.0 / H2)
                tile = turn(jnp.where(lane[:8] % 16 == 0, tile, 0.0), 2 * THICK - g)
                total = tile if total is None else total + tile
            moved[t] = total
            move_copy(t).start()

        for t in range(STEPS):
            floor_ref[0, t] = dense(arrived[t, 0:8], 1)
            move_copy(t).wait_send()

    for dx, dy in DIRS:
        @pl.when(exists(dx, dy))
        def _(dx=dx, dy=dy):
            for copy in halo_copies(dx, dy):
                copy.wait_send()

            @pl.when(wet)
            def _():
                prior_copy(dx, dy).wait_send()


def on_device(sizes, current, previous, material, prior):
    own = current.shape[2]
    own_tiles = own // LANES
    groups = own_tiles // PERIOD
    cells = own // PLANES
    field = pltpu.VMEM((ROWS, (own_tiles + 2 * PAD) * LANES), jnp.float32)
    pattern = pltpu.VMEM((ROWS, PERIOD * LANES), jnp.float32)
    anywhere = pl.BlockSpec(memory_space=pl.ANY)
    near = pl.BlockSpec(memory_space=pltpu.VMEM)
    dma = pltpu.SemaphoreType.DMA
    return pl.pallas_call(
        functools.partial(kernel, sizes, own_tiles),
        out_shape=(
            jax.ShapeDtypeStruct(current.shape, jnp.float32),
            jax.ShapeDtypeStruct((1,) + prior.shape, jnp.float32),
        ),
        in_specs=[anywhere] * 4,
        out_specs=(near, near),
        scratch_shapes=[field] * 8
        + [
            pltpu.VMEM((ROWS, PERIOD * LANES), jnp.int32),
            pattern,
            pattern,
            pltpu.VMEM(prior.shape, jnp.float32),
            pltpu.VMEM((len(DIRS), STEPS - 1) + prior.shape[1:], jnp.float32),
            pltpu.VMEM((STEPS, ROWS, LANES), jnp.float32),
            pltpu.VMEM((STEPS, ROWS, LANES), jnp.float32),
            pltpu.VMEM((STEPS, ROWS, (groups + 2) * LANES), jnp.float32),
            pltpu.VMEM((8, groups * LANES), jnp.float32),
            pltpu.VMEM((STEPS, 8, LANES), jnp.float32),
            pltpu.VMEM((STEPS, 8, LANES), jnp.float32),
            dma((4,)),
            dma((3 * len(DIRS),)),
            dma((3 * len(DIRS),)),
            dma((len(DIRS),)),
            dma((len(DIRS),)),
            dma((STEPS,)),
            dma((STEPS,)),
            dma((STEPS,)),
            dma((STEPS,)),
        ],
        compiler_params=pltpu.CompilerParams(collective_id=0, has_side_effects=True),
    )(current, previous, material, prior)


def solution(mesh):
    placed = (
        P("half", "gx", "gy"),
        P("half", "gx", "gy"),
        P("half", "gx", "gy"),
        P(None, "gx", "gy"),
    )
    return jax.shard_map(
        functools.partial(on_device, (mesh.shape["gx"], mesh.shape["gy"])),
        mesh=mesh,
        in_specs=placed,
        out_specs=(P("half", "gx", "gy"), P("half", None, "gx", "gy")),
        check_vma=False,
    )
```

```python
import functools

import jax
import jax.numpy as jnp
from jax import lax
from jax.experimental import pallas as pl
from jax.experimental.pallas import tpu as pltpu
from jax.sharding import PartitionSpec as P

STEPS = 4
PLANES = 144
THICK = PLANES // 3
TIME_STEP = 0.22
RELAXATION = 0.5
H2 = TIME_STEP * TIME_STEP

LANES = 128
ROWS = 16
PAD = 8
SPAN = 2
HALVES = 16
SLOTS = HALVES + 2 * STEPS
PERIOD = 9
MESH = pl.DeviceIdType.MESH
DIRS = tuple((dx, dy) for dx in (-1, 0, 1) for dy in (-1, 0, 1) if (dx, dy) != (0, 0))


def lanes_of(tile, count=1):
    start = (tile + PAD) * LANES
    if not isinstance(start, int):
        start = pl.multiple_of(start, LANES)
    return pl.ds(start, count * LANES)


def rows_sent(dx):
    return {0: pl.ds(0, 8), 1: pl.ds(4, 4), -1: pl.ds(0, 4)}[dx]


def rows_landed(dx):
    return {0: pl.ds(0, 8), 1: pl.ds(12, 4), -1: pl.ds(8, 4)}[dx]


def shift_x(value, by):
    return pltpu.roll(value, (-by) % ROWS, 0)


def turn(value, by):
    return pltpu.roll(value, (-by) % LANES, 1)


class Tiles:
    def __init__(self):
        self.known = {}

    def get(self, name, tile, make):
        key = (name, tile)
        if key not in self.known:
            self.known[key] = make()
        return self.known[key]


def flat_shift(memo, name, of, lane, tile, by):
    whole, part = divmod(by, LANES)
    first = memo.get(("turn", name, part), tile + whole, lambda: turn(of(tile + whole), part))
    if part == 0:
        return first
    second = memo.get(("turn", name, part), tile + whole + 1, lambda: turn(of(tile + whole + 1), part))
    return jnp.where(lane < LANES - part, first, second)


def unit_window(memo, of, lane, start, low, high):
    tile, part = divmod(start, LANES)
    if part + low >= LANES:
        tile, part, low, high = tile + 1, part - LANES, low, high
    first = memo.get("turn", (tile, part % LANES), lambda: turn(of(tile), part % LANES))
    if part + high <= LANES:
        return first
    second = memo.get("turn", (tile + 1, part % LANES), lambda: turn(of(tile + 1), part % LANES))
    return jnp.where(lane < LANES - part, first, second)


def to_planes(ref, rows, slots, base, store):
    memo = Tiles()
    lane = lax.broadcasted_iota(jnp.int32, (8, LANES), 1)

    def of(tile):
        return memo.get("load", tile, lambda: ref[rows, lanes_of(base + tile)])

    for slot in slots:
        parts = []
        for c in range(3):
            near = (slot - STEPS) * PLANES + c * THICK
            far = near + HALVES * PLANES - THICK
            parts.append(
                jnp.where(
                    lane < THICK,
                    unit_window(memo, of, lane, near, 0, THICK),
                    unit_window(memo, of, lane, far, THICK, 2 * THICK),
                )
            )
        store(slot, parts)


def from_planes(planes, dst, tiles):
    lane = lax.broadcasted_iota(jnp.int32, (8, LANES), 1)
    for q in tiles:
        out = None
        for n in range(q * LANES // THICK, (q * LANES + LANES - 1) // THICK + 1):
            cell, c = divmod(n, 3)
            far = cell >= HALVES
            slot = cell + STEPS - (HALVES if far else 0)
            value = turn(planes[slot, c, 0:8], q * LANES - n * THICK + (THICK if far else 0))
            out = value if out is None else jnp.where(lane < n * THICK - q * LANES, out, value)
        dst[:, pl.ds(q * LANES, LANES)] = out


def slopes(src, level, slot, sz, sx, ex, ez, lap, rows):
    lane = lax.broadcasted_iota(jnp.int32, (ROWS, LANES), 1)
    keep_up = jnp.where((lane == THICK - 1) | (lane >= 2 * THICK - 1), 0.0, 1.0)
    keep_down = jnp.where((lane == 0) | (lane == THICK), 0.0, 1.0)
    lap_x, lap_z, mixed = [], [], []
    for c in range(3):
        u = src[slot, c]
        up, down = turn(u, 1) * keep_up, turn(u, -1) * keep_down
        right, left = shift_x(u, 1)[:rows], shift_x(u, -1)[:rows]
        slope_z = (up - down) * 0.25
        lap_z.append((up + down)[:rows])
        lap_x.append(right + left)
        if c < 2:
            sx[level, slot, c, 0:rows] = (right - left) * 0.25
        if c > 0:
            sz[level, slot, c - 1, 0:rows] = slope_z[:rows]
        if c != 1:
            mixed.append((shift_x(slope_z, 1) - shift_x(slope_z, -1))[:rows])
        lap[level, slot, c, 0:rows] = lap_x[c] + lap_z[c]
    ex[level, slot, 0:rows] = lap_x[0] + mixed[1]
    ez[level, slot, 0:rows] = lap_z[2] + mixed[0]


def advance_slot(src, old, dst, level, slot, sz, sx, ex, ez, lap, stiff, pushed, rows):
    bulk, shear, light = (stiff[slot, n, 0:rows] for n in range(3))
    centre = [src[slot, c, 0:rows] for c in range(3)]
    lap_y = [src[slot + 1, c, 0:rows] + src[slot - 1, c, 0:rows] for c in range(3)]

    def along(ref, c):
        return ref[level, slot + 1, c, 0:rows] - ref[level, slot - 1, c, 0:rows]

    grad = (
        ex[level, slot, 0:rows] + along(sx, 1),
        lap_y[1] + (along(sx, 0) + along(sz, 1)),
        ez[level, slot, 0:rows] + along(sz, 0),
    )
    for c in range(3):
        twice = centre[c] + centre[c]
        total = lap[level, slot, c, 0:rows] + lap_y[c] - 6.0 * centre[c]
        acc = bulk * (grad[c] - twice) + shear * total
        if c == 2:
            acc = acc + light * pushed
        dst[slot, c, 0:rows] = twice - old[slot, c, 0:rows] + acc
    return acc


def water_block(src, old, dst, mod, ghost, dst_pad, base, tiles, last):
    memo = Tiles()
    lane = lax.broadcasted_iota(jnp.int32, (ROWS, LANES), 1)
    rows = 8 if last else ROWS

    def at(ref, j):
        return ref[:, lanes_of(base + j)]

    def u(j):
        return memo.get("u", j, lambda: at(src, j))

    for j in tiles:
        below = flat_shift(memo, "u", u, lane, j, 1)
        above = flat_shift(memo, "u", u, lane, j, -1)
        offset = (j * LANES) % PLANES
        top = (-offset) % PLANES
        floor = PLANES - 1 - offset
        if top < LANES:
            above = jnp.where(lane == top, 0.0, above)
        if 0 <= floor < LANES:
            below = jnp.where(lane == floor, u(j) - ghost(j), below)
        total = (shift_x(u(j), 1) + shift_x(u(j), -1)) + (below + above)
        total = total + (flat_shift(memo, "u", u, lane, j, PLANES) + flat_shift(memo, "u", u, lane, j, -PLANES))
        total = (total - 6.0 * u(j))[:rows]
        centre = u(j)[:rows]
        new = (centre + centre) - at(old, j)[:rows] + (H2 * at(mod, j)[:rows]) * total
        if last:
            dst[:, pl.ds(dst_pad + j * LANES, LANES)] = new
        else:
            dst[:, lanes_of(base + j)] = new


def floor_lane(tile):
    if tile % PERIOD == 0:
        return None
    return (tile - 1) // PERIOD, 16 * ((tile - 1) % PERIOD) + 15


def exact_dot(a, b):
    return jnp.dot(a, b, precision=lax.Precision.HIGHEST, preferred_element_type=jnp.float32)


def kernel(
    sizes, own_tiles, cur_hbm, prev_hbm, mat_hbm, prior_hbm, fields_ref, floor_ref,
    cur, prev, mat, p1, p2, p3, d0, d1, d2, d3, d4, before, stiff, sz, sx, ex, ez, lap,
    prior, rims, packed, arrived, spread, moved, returned,
    load_sem, send_sem, recv_sem, prior_send, prior_recv, trace_send, trace_recv, move_send, move_recv,
):
    half, gx, gy = lax.axis_index("half"), lax.axis_index("gx"), lax.axis_index("gy")
    n_x, n_y = sizes
    wet = half == 0
    groups = own_tiles // PERIOD

    def exists(dx, dy):
        x, y = gx + dx, gy + dy
        return (x >= 0) & (x < n_x) & (y >= 0) & (y < n_y)

    loads = [
        pltpu.make_async_copy(src.at[0], dst.at[0:8, lanes_of(0, own_tiles)], load_sem.at[n])
        for n, (src, dst) in enumerate(((cur_hbm, cur), (prev_hbm, prev), (mat_hbm, mat)))
    ]
    loads.append(pltpu.make_async_copy(prior_hbm, prior, load_sem.at[3]))
    for copy in loads:
        copy.start()

    barrier = pltpu.get_barrier_semaphore()
    count = jnp.int32(1)
    for dx, dy in DIRS:
        here = exists(dx, dy)
        count = count + here.astype(jnp.int32)

        @pl.when(here)
        def _(dx=dx, dy=dy):
            pl.semaphore_signal(barrier, inc=1, device_id={"gx": gx + dx, "gy": gy + dy}, device_id_type=MESH)

    pl.semaphore_signal(barrier, inc=1, device_id={"half": 1 - half}, device_id_type=MESH)

    def halo_copies(dx, dy):
        out = []
        for n, (ref, width) in enumerate(((cur, 5), (prev, 4), (mat, 4))):
            if dy == 0:
                src_lanes = dst_lanes = lanes_of(0, own_tiles)
            elif dy == 1:
                src_lanes, dst_lanes = lanes_of(own_tiles - width, width), lanes_of(-width, width)
            else:
                src_lanes, dst_lanes = lanes_of(0, width), lanes_of(own_tiles, width)
            slot = DIRS.index((dx, dy)) * 3 + n
            out.append(
                pltpu.make_async_remote_copy(
                    src_ref=ref.at[rows_sent(dx), src_lanes],
                    dst_ref=ref.at[rows_landed(dx), dst_lanes],
                    send_sem=send_sem.at[slot],
                    recv_sem=recv_sem.at[slot],
                    device_id={"gx": gx + dx, "gy": gy + dy},
                    device_id_type=MESH,
                )
            )
        return out

    def prior_copy(dx, dy):
        slot = DIRS.index((dx, dy))
        return pltpu.make_async_remote_copy(
            src_ref=prior.at[pl.ds(0, STEPS - 1)],
            dst_ref=rims.at[slot],
            send_sem=prior_send.at[slot],
            recv_sem=prior_recv.at[slot],
            device_id={"gx": gx + dx, "gy": gy + dy},
            device_id_type=MESH,
        )

    for dx, dy in DIRS:
        @pl.when(jnp.logical_not(exists(-dx, -dy)))
        def _(dx=dx, dy=dy):
            lanes = {0: lanes_of(0, own_tiles), 1: lanes_of(-5, 5), -1: lanes_of(own_tiles, 5)}[dy]
            for ref in (cur, prev, mat):
                ref[rows_landed(dx), lanes] = jnp.zeros((8 if dx == 0 else 4, lanes.size), jnp.float32)
            rims[DIRS.index((dx, dy))] = jnp.zeros(rims.shape[1:], jnp.float32)

    for copy in loads:
        copy.wait()
    pl.semaphore_wait(barrier, count)

    order = sorted(DIRS, key=lambda d: (d[1] == 0, d[0] != 0))
    for dx, dy in order:
        @pl.when(exists(dx, dy))
        def _(dx=dx, dy=dy):
            for copy in halo_copies(dx, dy):
                copy.start()

            @pl.when(wet)
            def _():
                prior_copy(dx, dy).start()

    for dx, dy in DIRS:
        @pl.when(exists(-dx, -dy))
        def _(dx=dx, dy=dy):
            for copy in halo_copies(dx, dy):
                copy.wait_recv()

            @pl.when(wet)
            def _():
                prior_copy(dx, dy).wait_recv()

    lane = lax.broadcasted_iota(jnp.int32, (ROWS, LANES), 1)
    levels = (cur, p1, p2, p3)
    olds = (prev, cur, p1, p2)
    width = own_tiles * LANES

    def over_tiles(block, t):
        margin = STEPS - 1 - t
        edge = -(-margin * PLANES // LANES)
        if edge:
            block(0, range(-edge, 0), 0)
        @pl.loop(0, groups)
        def _(g):
            block(g * PERIOD, range(PERIOD), g + 1)

        if edge:
            block(own_tiles, range(edge), groups + 1)

    def trace_copy(t):
        return pltpu.make_async_remote_copy(
            src_ref=packed.at[t], dst_ref=arrived.at[t], send_sem=trace_send.at[t], recv_sem=trace_recv.at[t],
            device_id={"half": 1 - half}, device_id_type=MESH,
        )

    def move_copy(t):
        return pltpu.make_async_remote_copy(
            src_ref=moved.at[t], dst_ref=returned.at[t], send_sem=move_send.at[t], recv_sem=move_recv.at[t],
            device_id={"half": 1 - half}, device_id_type=MESH,
        )

    def dense(value, first):
        cells = 8 * groups
        row = lax.broadcasted_iota(jnp.int32, (LANES, cells), 0)
        col = lax.broadcasted_iota(jnp.int32, (LANES, cells), 1)
        pick = (row == 16 * (col % 8) + first + col // 8).astype(jnp.float32)
        return exact_dot(value, pick)

    @pl.when(wet)
    def _():
        cells = 8 * groups
        row = lax.broadcasted_iota(jnp.int32, (cells, groups * LANES), 0)
        col = lax.broadcasted_iota(jnp.int32, (cells, groups * LANES), 1)
        place = (col == LANES * (row // 8) + 16 * (row % 8) + 15).astype(jnp.float32)
        upper = lax.broadcasted_iota(jnp.int32, (8, cells), 0) < 4

        def rim(dx, dy, t):
            return rims[DIRS.index((dx, dy)), t]

        for t in range(STEPS):
            centre = prior[t]
            if t == STEPS - 1:
                spread[t, 0:8, pl.ds(LANES, groups * LANES)] = exact_dot(centre, place)
                continue
            for dy, value in (
                (0, jnp.concatenate([centre, jnp.where(upper, rim(-1, 0, t), rim(1, 0, t))], 0)),
                (1, jnp.concatenate([rim(0, 1, t), jnp.where(upper, rim(-1, 1, t), rim(1, 1, t))], 0)),
                (-1, jnp.concatenate([rim(0, -1, t), jnp.where(upper, rim(-1, -1, t), rim(1, -1, t))], 0)),
            ):
                if dy == 0:
                    spread[t, :, pl.ds(LANES, groups * LANES)] = exact_dot(value, place)
                elif dy == 1:
                    spread[t, :, pl.ds(0, LANES)] = exact_dot(value, place[:, (groups - 1) * LANES:])
                else:
                    spread[t, :, pl.ds((groups + 1) * LANES, LANES)] = exact_dot(value, place[:, :LANES])

        for t in range(STEPS):
            src, old = levels[t], olds[t]
            margin = STEPS - 1 - t
            total = None
            for g in range(-1, groups + 1):
                tile = None
                for j in range(8):
                    q = g * PERIOD + j + 1
                    edge = -(-margin * PLANES // LANES)
                    if q < -edge or q >= own_tiles + edge:
                        continue
                    value = src[:, lanes_of(q)]
                    tile = value if tile is None else jnp.where(lane == 16 * j + 15, value, tile)
                if tile is None:
                    continue
                tile = jnp.where(lane % 16 == 15, tile, 0.0)
                tile = turn(tile, 15 - (g + 1))
                total = tile if total is None else total + tile
            packed[t] = total
            trace_copy(t).start()

            def block(base, tiles, slot, t=t, src=src, old=old):
                last = t == STEPS - 1
                start = 0
                if last:
                    start = pl.multiple_of(base * LANES, LANES)

                def ghost(j):
                    at = slot * LANES
                    if not isinstance(at, int):
                        at = pl.multiple_of(at, LANES)
                    return spread[t, :, pl.ds(at, LANES)]

                dst = fields_ref.at[0] if last else levels[t + 1]
                water_block(src, old, dst, mat, ghost, start, base, tiles, last)

            over_tiles(block, t)

        for t in range(STEPS):
            move_copy(t).wait_recv()
            motion = jnp.where(lane[:8] < HALVES, returned[t], turn(returned[t], THICK - HALVES))
            floor_ref[0, t] = RELAXATION * motion[:, : 8 * groups] + (1.0 - RELAXATION) * prior[t]
            trace_copy(t).wait_send()

    @pl.when(jnp.logical_not(wet))
    def _():
        def convert(rows, slots, base=0, shift=0):
            def put(ref):
                def store(slot, parts):
                    for c in range(3):
                        ref[slot + shift, c, rows] = parts[c]
                return store

            def put_stiff(slot, parts):
                light = H2 * parts[2]
                stiff[slot + shift, 0, rows] = light * parts[0]
                stiff[slot + shift, 1, rows] = light * parts[1]
                stiff[slot + shift, 2, rows] = light

            inner = [slot for slot in slots if 0 < slot < SLOTS - 1]
            to_planes(cur, rows, slots, base, put(d0))
            to_planes(prev, rows, inner, base, put(before))
            to_planes(mat, rows, inner, base, put_stiff)

        for rows in (pl.ds(0, 8), pl.ds(8, 8)):
            @pl.loop(0, HALVES // 8)
            def _(n, rows=rows):
                convert(rows, range(STEPS, STEPS + 8), n * PERIOD, n * 8)

            convert(rows, (*range(STEPS), *range(SLOTS - STEPS, SLOTS)))

        displaced = (d0, d1, d2, d3, d4)
        earlier = (before, d0, d1, d2)
        scratch = (sz, sx, ex, ez, lap)
        lane8 = lane[:8]

        for t in range(STEPS):
            last = t == STEPS - 1
            rows = 8 if last else ROWS
            src, old, dst = displaced[t], earlier[t], displaced[t + 1]

            @pl.loop(t, SLOTS - t, step=SPAN)
            def _(first, t=t, src=src, rows=rows):
                for k in range(SPAN):
                    slopes(src, t, first + k, *scratch, rows)

            trace_copy(t).wait_recv()
            load = arrived[t][:rows]
            lane_out = lane[:rows]

            def pushed(slot, load=load, lane_out=lane_out):
                cell = slot - STEPS
                near = cell % 8 * 16 + 1 + cell // 8
                return jnp.where(
                    lane_out == 0, turn(load, near),
                    jnp.where(lane_out == THICK, turn(load, near + HALVES // 8 - THICK), 0.0),
                )

            total = jnp.zeros((8, LANES), jnp.float32)
            for slot in range(t + 1, SLOTS - 1 - t):
                acc = advance_slot(src, old, dst, t, slot, *scratch, stiff, pushed(slot), rows)
                cell = slot - STEPS
                if 0 <= cell < HALVES:
                    total = jnp.where((lane8 == cell) | (lane8 == THICK + cell), turn(acc[:8], -cell), total)
            moved[t] = total * (1.0 / H2)
            move_copy(t).start()

        from_planes(d4, fields_ref.at[0], range(own_tiles))
        for t in range(STEPS):
            floor_ref[0, t] = dense(arrived[t, 0:8], 1)
            move_copy(t).wait_send()

    for dx, dy in DIRS:
        @pl.when(exists(dx, dy))
        def _(dx=dx, dy=dy):
            for copy in halo_copies(dx, dy):
                copy.wait_send()

            @pl.when(wet)
            def _():
                prior_copy(dx, dy).wait_send()


def on_device(sizes, current, previous, material, prior):
    own = current.shape[2]
    own_tiles = own // LANES
    groups = own_tiles // PERIOD
    cells = own // PLANES
    field = pltpu.VMEM((ROWS, (own_tiles + 2 * PAD) * LANES), jnp.float32)
    planes = pltpu.VMEM((SLOTS, 3, ROWS, LANES), jnp.float32)

    def per_level(count):
        return pltpu.VMEM((STEPS, SLOTS) + count + (ROWS, LANES), jnp.float32)

    anywhere = pl.BlockSpec(memory_space=pl.ANY)
    near = pl.BlockSpec(memory_space=pltpu.VMEM)
    dma = pltpu.SemaphoreType.DMA
    return pl.pallas_call(
        functools.partial(kernel, sizes, own_tiles),
        out_shape=(
            jax.ShapeDtypeStruct(current.shape, jnp.float32),
            jax.ShapeDtypeStruct((1,) + prior.shape, jnp.float32),
        ),
        in_specs=[anywhere] * 4,
        out_specs=(near, near),
        scratch_shapes=[field] * 6
        + [planes] * 7
        + [per_level((2,)), per_level((2,)), per_level(()), per_level(()), per_level((3,))]
        + [
            pltpu.VMEM(prior.shape, jnp.float32),
            pltpu.VMEM((len(DIRS), STEPS - 1) + prior.shape[1:], jnp.float32),
            pltpu.VMEM((STEPS, ROWS, LANES), jnp.float32),
            pltpu.VMEM((STEPS, ROWS, LANES), jnp.float32),
            pltpu.VMEM((STEPS, ROWS, (groups + 2) * LANES), jnp.float32),
            pltpu.VMEM((STEPS, 8, LANES), jnp.float32),
            pltpu.VMEM((STEPS, 8, LANES), jnp.float32),
            dma((4,)),
            dma((3 * len(DIRS),)),
            dma((3 * len(DIRS),)),
            dma((len(DIRS),)),
            dma((len(DIRS),)),
            dma((STEPS,)),
            dma((STEPS,)),
            dma((STEPS,)),
            dma((STEPS,)),
        ],
        compiler_params=pltpu.CompilerParams(collective_id=0, has_side_effects=True),
    )(current, previous, material, prior)


def solution(mesh):
    placed = (
        P("half", "gx", "gy"),
        P("half", "gx", "gy"),
        P("half", "gx", "gy"),
        P(None, "gx", "gy"),
    )
    return jax.shard_map(
        functools.partial(on_device, (mesh.shape["gx"], mesh.shape["gy"])),
        mesh=mesh,
        in_specs=placed,
        out_specs=(P("half", "gx", "gy"), P("half", None, "gx", "gy")),
        check_vma=False,
    )
```

```python
import functools

import jax
import jax.numpy as jnp
from jax import lax
from jax.experimental import pallas as pl
from jax.experimental.pallas import tpu as pltpu
from jax.sharding import PartitionSpec as P

STEPS = 4
PLANES = 144
THICK = PLANES // 3
TIME_STEP = 0.22
RELAXATION = 0.5
H2 = TIME_STEP * TIME_STEP

LANES = 128
ROWS = 16
PAD = 8
HALVES = 16
SLOTS = HALVES + 2 * STEPS
PERIOD = 9
MESH = pl.DeviceIdType.MESH
DIRS = tuple((dx, dy) for dx in (-1, 0, 1) for dy in (-1, 0, 1) if (dx, dy) != (0, 0))


def lanes_of(tile, count=1):
    start = (tile + PAD) * LANES
    if not isinstance(start, int):
        start = pl.multiple_of(start, LANES)
    return pl.ds(start, count * LANES)


def rows_sent(dx, depth):
    return {0: pl.ds(0, 8), 1: pl.ds(8 - depth, depth), -1: pl.ds(0, depth)}[dx]


def rows_landed(dx, depth):
    return {0: pl.ds(0, 8), 1: pl.ds(16 - depth, depth), -1: pl.ds(8, depth)}[dx]


def shift_x(value, by):
    return pltpu.roll(value, (-by) % ROWS, 0)


def turn(value, by):
    return pltpu.roll(value, (-by) % LANES, 1)


class Tiles:
    def __init__(self):
        self.known = {}

    def get(self, name, tile, make):
        key = (name, tile)
        if key not in self.known:
            self.known[key] = make()
        return self.known[key]


def flat_shift(memo, name, of, lane, tile, by):
    whole, part = divmod(by, LANES)
    first = memo.get(("turn", name, part), tile + whole, lambda: turn(of(tile + whole), part))
    if part == 0:
        return first
    second = memo.get(("turn", name, part), tile + whole + 1, lambda: turn(of(tile + whole + 1), part))
    return jnp.where(lane < LANES - part, first, second)


def unit_window(memo, of, lane, start, low, high):
    tile, part = divmod(start, LANES)
    if part + low >= LANES:
        tile, part, low, high = tile + 1, part - LANES, low, high
    first = memo.get("turn", (tile, part % LANES), lambda: turn(of(tile), part % LANES))
    if part + high <= LANES:
        return first
    second = memo.get("turn", (tile + 1, part % LANES), lambda: turn(of(tile + 1), part % LANES))
    return jnp.where(lane < LANES - part, first, second)


def to_planes(ref, rows, slots, base, store):
    memo = Tiles()
    lane = lax.broadcasted_iota(jnp.int32, (8, LANES), 1)

    def of(tile):
        return memo.get("load", tile, lambda: ref[rows, lanes_of(base + tile)])

    for slot in slots:
        parts = []
        for c in range(3):
            near = (slot - STEPS) * PLANES + c * THICK
            far = near + HALVES * PLANES - THICK
            parts.append(
                jnp.where(
                    lane < THICK,
                    unit_window(memo, of, lane, near, 0, THICK),
                    unit_window(memo, of, lane, far, THICK, 2 * THICK),
                )
            )
        store(slot, parts)


def from_planes(planes, dst, tiles):
    lane = lax.broadcasted_iota(jnp.int32, (8, LANES), 1)
    for q in tiles:
        out = None
        for n in range(q * LANES // THICK, (q * LANES + LANES - 1) // THICK + 1):
            cell, c = divmod(n, 3)
            far = cell >= HALVES
            slot = cell + STEPS - (HALVES if far else 0)
            value = turn(planes[slot, c, 0:8], q * LANES - n * THICK + (THICK if far else 0))
            out = value if out is None else jnp.where(lane < n * THICK - q * LANES, out, value)
        dst[:, pl.ds(q * LANES, LANES)] = out


def slopes(src, level, slot, sz, sx, ex, ez, lap, rows):
    lane = lax.broadcasted_iota(jnp.int32, (ROWS, LANES), 1)
    keep_up = jnp.where((lane == THICK - 1) | (lane >= 2 * THICK - 1), 0.0, 1.0)
    keep_down = jnp.where((lane == 0) | (lane == THICK), 0.0, 1.0)
    lap_x, lap_z, mixed = [], [], []
    for c in range(3):
        u = src[slot, c]
        up, down = turn(u, 1) * keep_up, turn(u, -1) * keep_down
        right, left = shift_x(u, 1)[:rows], shift_x(u, -1)[:rows]
        slope_z = (up - down) * 0.25
        lap_z.append((up + down)[:rows])
        lap_x.append(right + left)
        if c < 2:
            sx[level, slot, c, 0:rows] = (right - left) * 0.25
        if c > 0:
            sz[level, slot, c - 1, 0:rows] = slope_z[:rows]
        if c != 1:
            mixed.append((shift_x(slope_z, 1) - shift_x(slope_z, -1))[:rows])
        lap[level, slot, c, 0:rows] = lap_x[c] + lap_z[c]
    ex[level, slot, 0:rows] = lap_x[0] + mixed[1]
    ez[level, slot, 0:rows] = lap_z[2] + mixed[0]


def advance_slot(src, old, dst, level, slot, sz, sx, ex, ez, lap, stiff, pushed, rows):
    bulk, shear, light = (stiff[slot, n, 0:rows] for n in range(3))
    centre = [src[slot, c, 0:rows] for c in range(3)]
    lap_y = [src[slot + 1, c, 0:rows] + src[slot - 1, c, 0:rows] for c in range(3)]

    def along(ref, c):
        return ref[level, slot + 1, c, 0:rows] - ref[level, slot - 1, c, 0:rows]

    grad = (
        ex[level, slot, 0:rows] + along(sx, 1),
        lap_y[1] + (along(sx, 0) + along(sz, 1)),
        ez[level, slot, 0:rows] + along(sz, 0),
    )
    for c in range(3):
        twice = centre[c] + centre[c]
        total = lap[level, slot, c, 0:rows] + lap_y[c] - 6.0 * centre[c]
        acc = bulk * (grad[c] - twice) + shear * total
        if c == 2:
            acc = acc + light * pushed
        dst[slot, c, 0:rows] = twice - old[slot, c, 0:rows] + acc
    return acc


def water_block(src, old, dst, mod, ghost, dst_pad, base, tiles, last):
    memo = Tiles()
    lane = lax.broadcasted_iota(jnp.int32, (ROWS, LANES), 1)
    rows = 8 if last else ROWS

    def at(ref, j):
        return ref[:, lanes_of(base + j)]

    def u(j):
        return memo.get("u", j, lambda: at(src, j))

    for j in tiles:
        below = flat_shift(memo, "u", u, lane, j, 1)
        above = flat_shift(memo, "u", u, lane, j, -1)
        offset = (j * LANES) % PLANES
        top = (-offset) % PLANES
        floor = PLANES - 1 - offset
        if top < LANES:
            above = jnp.where(lane == top, 0.0, above)
        if 0 <= floor < LANES:
            below = jnp.where(lane == floor, u(j) - ghost(j), below)
        total = (shift_x(u(j), 1) + shift_x(u(j), -1)) + (below + above)
        total = total + (flat_shift(memo, "u", u, lane, j, PLANES) + flat_shift(memo, "u", u, lane, j, -PLANES))
        total = (total - 6.0 * u(j))[:rows]
        centre = u(j)[:rows]
        new = (centre + centre) - at(old, j)[:rows] + (H2 * at(mod, j)[:rows]) * total
        if last:
            dst[:, pl.ds(dst_pad + j * LANES, LANES)] = new
        else:
            dst[:, lanes_of(base + j)] = new


def floor_lane(tile):
    if tile % PERIOD == 0:
        return None
    return (tile - 1) // PERIOD, 16 * ((tile - 1) % PERIOD) + 15


def exact_dot(a, b):
    return jnp.dot(a, b, precision=lax.Precision.HIGHEST, preferred_element_type=jnp.float32)


def kernel(
    sizes, own_tiles, cur_hbm, prev_hbm, mat_hbm, prior_hbm, fields_ref, floor_ref,
    cur, prev, mat, p1, p2, p3, d0, d1, d2, d3, d4, before, stiff, sz, sx, ex, ez, lap,
    prior, outgoing, rims, packed, arrived, spread, moved, returned,
    load_sem, send_sem, recv_sem, prior_send, prior_recv, trace_send, trace_recv, move_send, move_recv,
):
    half, gx, gy = lax.axis_index("half"), lax.axis_index("gx"), lax.axis_index("gy")
    n_x, n_y = sizes
    wet = half == 0
    groups = own_tiles // PERIOD

    def exists(dx, dy):
        x, y = gx + dx, gy + dy
        return (x >= 0) & (x < n_x) & (y >= 0) & (y < n_y)

    loads = [
        pltpu.make_async_copy(src.at[0], dst.at[0:8, lanes_of(0, own_tiles)], load_sem.at[n])
        for n, (src, dst) in enumerate(((cur_hbm, cur), (prev_hbm, prev), (mat_hbm, mat)))
    ]
    loads.append(pltpu.make_async_copy(prior_hbm, prior, load_sem.at[3]))
    for copy in loads:
        copy.start()

    barrier = pltpu.get_barrier_semaphore()
    count = jnp.int32(1)
    for dx, dy in DIRS:
        here = exists(dx, dy)
        count = count + here.astype(jnp.int32)

        @pl.when(here)
        def _(dx=dx, dy=dy):
            pl.semaphore_signal(barrier, inc=1, device_id={"gx": gx + dx, "gy": gy + dy}, device_id_type=MESH)

    pl.semaphore_signal(barrier, inc=1, device_id={"half": 1 - half}, device_id_type=MESH)

    def halo_copies(dx, dy):
        out = []
        for n, (ref, depth) in enumerate(((cur, STEPS), (prev, STEPS - 1), (mat, STEPS - 1))):
            width = -(-depth * PLANES // LANES)
            if dy == 0:
                src_lanes = dst_lanes = lanes_of(0, own_tiles)
            elif dy == 1:
                src_lanes, dst_lanes = lanes_of(own_tiles - width, width), lanes_of(-width, width)
            else:
                src_lanes, dst_lanes = lanes_of(0, width), lanes_of(own_tiles, width)
            slot = DIRS.index((dx, dy)) * 3 + n
            out.append(
                pltpu.make_async_remote_copy(
                    src_ref=ref.at[rows_sent(dx, depth), src_lanes],
                    dst_ref=ref.at[rows_landed(dx, depth), dst_lanes],
                    send_sem=send_sem.at[slot],
                    recv_sem=recv_sem.at[slot],
                    device_id={"gx": gx + dx, "gy": gy + dy},
                    device_id_type=MESH,
                )
            )
        return out

    def prior_copy(dx, dy):
        slot = DIRS.index((dx, dy))
        return pltpu.make_async_remote_copy(
            src_ref=outgoing.at[rows_sent(dx, STEPS)],
            dst_ref=rims.at[slot, rows_landed(dx, STEPS) if dx == 0 else rows_sent(dx, STEPS)],
            send_sem=prior_send.at[slot],
            recv_sem=prior_recv.at[slot],
            device_id={"gx": gx + dx, "gy": gy + dy},
            device_id_type=MESH,
        )

    for dx, dy in DIRS:
        @pl.when(jnp.logical_not(exists(-dx, -dy)))
        def _(dx=dx, dy=dy):
            lanes = {0: lanes_of(0, own_tiles), 1: lanes_of(-5, 5), -1: lanes_of(own_tiles, 5)}[dy]
            for ref in (cur, prev, mat):
                ref[rows_landed(dx, STEPS), lanes] = jnp.zeros((8 if dx == 0 else 4, lanes.size), jnp.float32)
            rims[DIRS.index((dx, dy))] = jnp.zeros(rims.shape[1:], jnp.float32)

    for copy in loads:
        copy.wait()
    cells = prior.shape[2]
    idle = jnp.zeros((8, LANES - (STEPS - 1) * cells), jnp.float32)
    outgoing[...] = jnp.concatenate([prior[t] for t in range(STEPS - 1)] + [idle], 1)
    pl.semaphore_wait(barrier, count)

    order = sorted(DIRS, key=lambda d: (d[1] == 0, d[0] != 0))
    for dx, dy in order:
        @pl.when(exists(dx, dy))
        def _(dx=dx, dy=dy):
            for copy in halo_copies(dx, dy):
                copy.start()

            @pl.when(wet)
            def _():
                prior_copy(dx, dy).start()

    def await_rim(dx, dy):
        @pl.when(exists(-dx, -dy))
        def _():
            for copy in halo_copies(dx, dy):
                copy.wait_recv()

            @pl.when(wet)
            def _():
                prior_copy(dx, dy).wait_recv()

    lane = lax.broadcasted_iota(jnp.int32, (ROWS, LANES), 1)
    levels = (cur, p1, p2, p3)
    olds = (prev, cur, p1, p2)
    width = own_tiles * LANES

    def over_tiles(block, t):
        edge = -(-(STEPS - 1 - t) * PLANES // LANES)
        block(range(-edge, own_tiles + edge))

    def trace_copy(t):
        return pltpu.make_async_remote_copy(
            src_ref=packed.at[t], dst_ref=arrived.at[t], send_sem=trace_send.at[t], recv_sem=trace_recv.at[t],
            device_id={"half": 1 - half}, device_id_type=MESH,
        )

    def move_copy(t):
        return pltpu.make_async_remote_copy(
            src_ref=moved.at[t], dst_ref=returned.at[t], send_sem=move_send.at[t], recv_sem=move_recv.at[t],
            device_id={"half": 1 - half}, device_id_type=MESH,
        )

    def dense(value, first):
        cells = 8 * groups
        row = lax.broadcasted_iota(jnp.int32, (LANES, cells), 0)
        col = lax.broadcasted_iota(jnp.int32, (LANES, cells), 1)
        pick = (row == 16 * (col % 8) + first + col // 8).astype(jnp.float32)
        return exact_dot(value, pick)

    @pl.when(wet)
    def _():
        for dx, dy in DIRS:
            await_rim(dx, dy)

        sixteenth = lane // 16
        blocks = range(-1, groups + 1)

        def deepest(ref, reach):
            tiles = {}
            for g in blocks:
                tile = None
                for j in range(8):
                    q = g * PERIOD + j + 1
                    if -STEPS <= q <= own_tiles + reach:
                        value = ref[:, lanes_of(q)]
                        tile = value if tile is None else jnp.where(sixteenth == j, value, tile)
                tiles[g] = tile
            return tiles

        floor_lanes = lane % 16 == 15

        def send_trace(t, tiles):
            total = None
            for g in blocks:
                tile = turn(jnp.where(floor_lanes, tiles[g], 0.0), 15 - (g + 1))
                total = tile if total is None else total + tile
            packed[t] = total
            trace_copy(t).start()

        now, then = deepest(cur, STEPS), deepest(prev, STEPS - 1)
        send_trace(0, now)

        row = lax.broadcasted_iota(jnp.int32, (cells, groups * LANES), 0)
        col = lax.broadcasted_iota(jnp.int32, (cells, groups * LANES), 1)
        place = (col == LANES * (row // 8) + 16 * (row % 8) + 15).astype(jnp.float32)
        upper = lax.broadcasted_iota(jnp.int32, (8, cells), 0) < 4

        def rim(dx, dy, t):
            return (outgoing[...] if dx == dy == 0 else rims[DIRS.index((dx, dy))])[:, t * cells : (t + 1) * cells]

        for dy, first, count in ((0, 0, groups), (1, groups - 1, 1), (-1, 0, 1)):
            rows = []
            for t in range(STEPS - 1):
                rows += [rim(0, dy, t), jnp.where(upper, rim(-1, dy, t), rim(1, dy, t))]
            value = exact_dot(jnp.concatenate(rows, 0), place[:, first * LANES : (first + count) * LANES])
            at = {0: 1, 1: 0, -1: groups + 1}[dy]
            for t in range(STEPS - 1):
                spread[t, :, pl.ds(at * LANES, count * LANES)] = value[t * ROWS : (t + 1) * ROWS]

        def ghost_tile(t, g):
            return spread[t, :, pl.ds((g + 1) * LANES, LANES)]

        speed = deepest(mat, STEPS - 1)
        for t in range(STEPS - 1):
            memo = Tiles()
            later = {}
            inside = {g: now[g] for g in blocks}
            inside[-2] = inside[groups + 1] = jnp.zeros((ROWS, LANES), jnp.float32)

            def of(g, inside=inside):
                return inside[g]

            for g in blocks:
                u = now[g]
                below = jnp.where(floor_lanes, u - ghost_tile(t, g), turn(u, 1))
                total = (shift_x(u, 1) + shift_x(u, -1)) + (below + turn(u, -1))
                total = total + (
                    flat_shift(memo, "u", of, lane, g, 16) + flat_shift(memo, "u", of, lane, g, -16)
                )
                later[g] = (u + u) - then[g] + (H2 * speed[g]) * (total - 6.0 * u)
            then, now = now, later
            send_trace(t + 1, now)

        spread[STEPS - 1, 0:8, pl.ds(LANES, groups * LANES)] = exact_dot(prior[STEPS - 1], place)

        for t in range(STEPS):
            src, old = levels[t], olds[t]
            last = t == STEPS - 1

            def block(tiles, t=t, src=src, old=old, last=last):
                def ghost(j):
                    return ghost_tile(t, (j - 1) // PERIOD)

                dst = fields_ref.at[0] if last else levels[t + 1]
                water_block(src, old, dst, mat, ghost, 0, 0, tiles, last)

            over_tiles(block, t)

        for t in range(STEPS):
            move_copy(t).wait_recv()
            motion = jnp.where(lane[:8] < HALVES, returned[t], turn(returned[t], THICK - HALVES))
            floor_ref[0, t] = RELAXATION * motion[:, : 8 * groups] + (1.0 - RELAXATION) * prior[t]
            trace_copy(t).wait_send()

    @pl.when(jnp.logical_not(wet))
    def _():
        def convert(rows, slots, base=0, shift=0):
            def put(ref):
                def store(slot, parts):
                    for c in range(3):
                        ref[slot + shift, c, rows] = parts[c]
                return store

            def put_stiff(slot, parts):
                light = H2 * parts[2]
                stiff[slot + shift, 0, rows] = light * parts[0]
                stiff[slot + shift, 1, rows] = light * parts[1]
                stiff[slot + shift, 2, rows] = light

            inner = [slot for slot in slots if 0 < slot < SLOTS - 1]
            to_planes(cur, rows, slots, base, put(d0))
            to_planes(prev, rows, inner, base, put(before))
            to_planes(mat, rows, inner, base, put_stiff)

        def convert_inner(rows):
            @pl.loop(0, HALVES // 8)
            def _(n):
                convert(rows, range(STEPS, STEPS + 8), n * PERIOD, n * 8)

        upper, lower = pl.ds(0, 8), pl.ds(8, 8)
        convert_inner(upper)
        for dx, dy in DIRS:
            if dy == 0:
                await_rim(dx, dy)
        convert_inner(lower)
        for dx, dy in DIRS:
            if dy != 0:
                await_rim(dx, dy)
        for rows in (upper, lower):
            convert(rows, (*range(STEPS), *range(SLOTS - STEPS, SLOTS)))

        displaced = (d0, d1, d2, d3, d4)
        earlier = (before, d0, d1, d2)
        scratch = (sz, sx, ex, ez, lap)
        lane8 = lane[:8]

        for t in range(STEPS):
            last = t == STEPS - 1
            rows = 8 if last else ROWS
            src, old, dst = displaced[t], earlier[t], displaced[t + 1]

            for slot in range(t, SLOTS - t):
                slopes(src, t, slot, *scratch, rows)

            trace_copy(t).wait_recv()
            load = arrived[t][:rows]
            lane_out = lane[:rows]

            def pushed(slot, load=load, lane_out=lane_out):
                cell = slot - STEPS
                near = cell % 8 * 16 + 1 + cell // 8
                return jnp.where(
                    lane_out == 0, turn(load, near),
                    jnp.where(lane_out == THICK, turn(load, near + HALVES // 8 - THICK), 0.0),
                )

            total = jnp.zeros((8, LANES), jnp.float32)
            for slot in range(t + 1, SLOTS - 1 - t):
                acc = advance_slot(src, old, dst, t, slot, *scratch, stiff, pushed(slot), rows)
                cell = slot - STEPS
                if 0 <= cell < HALVES:
                    total = jnp.where((lane8 == cell) | (lane8 == THICK + cell), turn(acc[:8], -cell), total)
            moved[t] = total * (1.0 / H2)
            move_copy(t).start()

        from_planes(d4, fields_ref.at[0], range(own_tiles))
        for t in range(STEPS):
            floor_ref[0, t] = dense(arrived[t, 0:8], 1)
            move_copy(t).wait_send()

    for dx, dy in DIRS:
        @pl.when(exists(dx, dy))
        def _(dx=dx, dy=dy):
            for copy in halo_copies(dx, dy):
                copy.wait_send()

            @pl.when(wet)
            def _():
                prior_copy(dx, dy).wait_send()


def deliver(fields_ref, floor_ref, fields_out, floor_out, sem):
    copies = [
        pltpu.make_async_copy(src, dst, sem.at[n])
        for n, (src, dst) in enumerate(((fields_ref, fields_out), (floor_ref, floor_out)))
    ]
    for copy in copies:
        copy.start()
    for copy in copies:
        copy.wait()


def on_device(sizes, current, previous, material, prior):
    own = current.shape[2]
    own_tiles = own // LANES
    groups = own_tiles // PERIOD
    cells = own // PLANES
    field = pltpu.VMEM((ROWS, (own_tiles + 2 * PAD) * LANES), jnp.float32)
    planes = pltpu.VMEM((SLOTS, 3, ROWS, LANES), jnp.float32)

    def per_level(count):
        return pltpu.VMEM((STEPS, SLOTS) + count + (ROWS, LANES), jnp.float32)

    anywhere = pl.BlockSpec(memory_space=pl.ANY)
    near = pl.BlockSpec(memory_space=pltpu.VMEM)
    dma = pltpu.SemaphoreType.DMA
    held = pl.pallas_call(
        functools.partial(kernel, sizes, own_tiles),
        out_shape=(
            pltpu.VMEM(current.shape, jnp.float32),
            pltpu.VMEM((1,) + prior.shape, jnp.float32),
        ),
        in_specs=[anywhere] * 4,
        out_specs=(near, near),
        scratch_shapes=[field] * 6
        + [planes] * 7
        + [per_level((2,)), per_level((2,)), per_level(()), per_level(()), per_level((3,))]
        + [
            pltpu.VMEM(prior.shape, jnp.float32),
            pltpu.VMEM((8, LANES), jnp.float32),
            pltpu.VMEM((len(DIRS), 8, LANES), jnp.float32),
            pltpu.VMEM((STEPS, ROWS, LANES), jnp.float32),
            pltpu.VMEM((STEPS, ROWS, LANES), jnp.float32),
            pltpu.VMEM((STEPS, ROWS, (groups + 2) * LANES), jnp.float32),
            pltpu.VMEM((STEPS, 8, LANES), jnp.float32),
            pltpu.VMEM((STEPS, 8, LANES), jnp.float32),
            dma((4,)),
            dma((3 * len(DIRS),)),
            dma((3 * len(DIRS),)),
            dma((len(DIRS),)),
            dma((len(DIRS),)),
            dma((STEPS,)),
            dma((STEPS,)),
            dma((STEPS,)),
            dma((STEPS,)),
        ],
        compiler_params=pltpu.CompilerParams(collective_id=0, has_side_effects=True),
    )(current, previous, material, prior)
    return pl.pallas_call(
        deliver,
        out_shape=tuple(jax.ShapeDtypeStruct(x.shape, x.dtype) for x in held),
        in_specs=[near] * 2,
        out_specs=(anywhere, anywhere),
        scratch_shapes=[dma((2,))],
    )(*(pltpu.with_memory_space_constraint(x, pltpu.VMEM) for x in held))


def solution(mesh):
    placed = (
        P("half", "gx", "gy"),
        P("half", "gx", "gy"),
        P("half", "gx", "gy"),
        P(None, "gx", "gy"),
    )
    return jax.shard_map(
        functools.partial(on_device, (mesh.shape["gx"], mesh.shape["gy"])),
        mesh=mesh,
        in_specs=placed,
        out_specs=(P("half", "gx", "gy"), P("half", None, "gx", "gy")),
        check_vma=False,
    )
```

```python
import functools

import jax
import jax.numpy as jnp
from jax import lax
from jax.experimental import pallas as pl
from jax.experimental.pallas import tpu as pltpu
from jax.sharding import PartitionSpec as P

STEPS = 4
PLANES = 144
THICK = PLANES // 3
TIME_STEP = 0.22
RELAXATION = 0.5
H2 = TIME_STEP * TIME_STEP

LANES = 128
ROWS = 16
PAD = 8
HALVES = 16
SLOTS = HALVES + 2 * STEPS
PERIOD = 9
MESH = pl.DeviceIdType.MESH
DIRS = tuple((dx, dy) for dx in (-1, 0, 1) for dy in (-1, 0, 1) if (dx, dy) != (0, 0))


def lanes_of(tile, count=1):
    start = (tile + PAD) * LANES
    if not isinstance(start, int):
        start = pl.multiple_of(start, LANES)
    return pl.ds(start, count * LANES)


def rows_sent(dx, depth):
    return {0: pl.ds(0, 8), 1: pl.ds(8 - depth, depth), -1: pl.ds(0, depth)}[dx]


def rows_landed(dx, depth):
    return {0: pl.ds(0, 8), 1: pl.ds(16 - depth, depth), -1: pl.ds(8, depth)}[dx]


def shift_x(value, by):
    return pltpu.roll(value, (-by) % ROWS, 0)


def turn(value, by):
    return pltpu.roll(value, (-by) % LANES, 1)


class Tiles:
    def __init__(self):
        self.known = {}

    def get(self, name, tile, make):
        key = (name, tile)
        if key not in self.known:
            self.known[key] = make()
        return self.known[key]


def flat_shift(memo, name, of, lane, tile, by):
    whole, part = divmod(by, LANES)
    first = memo.get(("turn", name, part), tile + whole, lambda: turn(of(tile + whole), part))
    if part == 0:
        return first
    second = memo.get(("turn", name, part), tile + whole + 1, lambda: turn(of(tile + whole + 1), part))
    return jnp.where(lane < LANES - part, first, second)


def unit_window(memo, of, lane, start, low, high):
    tile, part = divmod(start, LANES)
    if part + low >= LANES:
        tile, part, low, high = tile + 1, part - LANES, low, high
    first = memo.get("turn", (tile, part % LANES), lambda: turn(of(tile), part % LANES))
    if part + high <= LANES:
        return first
    second = memo.get("turn", (tile + 1, part % LANES), lambda: turn(of(tile + 1), part % LANES))
    return jnp.where(lane < LANES - part, first, second)


def to_planes(ref, rows, slots, base, store):
    memo = Tiles()
    lane = lax.broadcasted_iota(jnp.int32, (8, LANES), 1)

    def of(tile):
        return memo.get("load", tile, lambda: ref[rows, lanes_of(base + tile)])

    for slot in slots:
        parts = []
        for c in range(3):
            near = (slot - STEPS) * PLANES + c * THICK
            far = near + HALVES * PLANES - THICK
            parts.append(
                jnp.where(
                    lane < THICK,
                    unit_window(memo, of, lane, near, 0, THICK),
                    unit_window(memo, of, lane, far, THICK, 2 * THICK),
                )
            )
        store(slot, parts)


def from_planes(planes, dst, tiles):
    lane = lax.broadcasted_iota(jnp.int32, (8, LANES), 1)
    for q in tiles:
        out = None
        for n in range(q * LANES // THICK, (q * LANES + LANES - 1) // THICK + 1):
            cell, c = divmod(n, 3)
            far = cell >= HALVES
            slot = cell + STEPS - (HALVES if far else 0)
            value = turn(planes[slot, c, 0:8], q * LANES - n * THICK + (THICK if far else 0))
            out = value if out is None else jnp.where(lane < n * THICK - q * LANES, out, value)
        dst[:, pl.ds(q * LANES, LANES)] = out


def slopes(src, level, slot, sz, sx, ex, ez, lap, rows):
    lane = lax.broadcasted_iota(jnp.int32, (ROWS, LANES), 1)
    keep_up = jnp.where((lane == THICK - 1) | (lane >= 2 * THICK - 1), 0.0, 1.0)
    keep_down = jnp.where((lane == 0) | (lane == THICK), 0.0, 1.0)
    lap_x, lap_z, mixed = [], [], []
    for c in range(3):
        u = src[slot, c]
        up, down = turn(u, 1) * keep_up, turn(u, -1) * keep_down
        right, left = shift_x(u, 1)[:rows], shift_x(u, -1)[:rows]
        slope_z = (up - down) * 0.25
        lap_z.append((up + down)[:rows])
        lap_x.append(right + left)
        if c < 2:
            sx[level, slot, c, 0:rows] = (right - left) * 0.25
        if c > 0:
            sz[level, slot, c - 1, 0:rows] = slope_z[:rows]
        if c != 1:
            mixed.append((shift_x(slope_z, 1) - shift_x(slope_z, -1))[:rows])
        lap[level, slot, c, 0:rows] = lap_x[c] + lap_z[c]
    ex[level, slot, 0:rows] = lap_x[0] + mixed[1]
    ez[level, slot, 0:rows] = lap_z[2] + mixed[0]


def advance_slot(src, old, dst, level, slot, sz, sx, ex, ez, lap, stiff, pushed, rows):
    bulk, shear, light = (stiff[slot, n, 0:rows] for n in range(3))
    centre = [src[slot, c, 0:rows] for c in range(3)]
    lap_y = [src[slot + 1, c, 0:rows] + src[slot - 1, c, 0:rows] for c in range(3)]

    def along(ref, c):
        return ref[level, slot + 1, c, 0:rows] - ref[level, slot - 1, c, 0:rows]

    grad = (
        ex[level, slot, 0:rows] + along(sx, 1),
        lap_y[1] + (along(sx, 0) + along(sz, 1)),
        ez[level, slot, 0:rows] + along(sz, 0),
    )
    for c in range(3):
        twice = centre[c] + centre[c]
        total = lap[level, slot, c, 0:rows] + lap_y[c] - 6.0 * centre[c]
        acc = bulk * (grad[c] - twice) + shear * total
        if c == 2:
            acc = acc + light * pushed
        dst[slot, c, 0:rows] = twice - old[slot, c, 0:rows] + acc
    return acc


def water_block(src, old, dst, mod, ghost, dst_pad, base, tiles, last):
    memo = Tiles()
    lane = lax.broadcasted_iota(jnp.int32, (ROWS, LANES), 1)
    rows = 8 if last else ROWS

    def at(ref, j):
        return ref[:, lanes_of(base + j)]

    def u(j):
        return memo.get("u", j, lambda: at(src, j))

    for j in tiles:
        below = flat_shift(memo, "u", u, lane, j, 1)
        above = flat_shift(memo, "u", u, lane, j, -1)
        offset = (j * LANES) % PLANES
        top = (-offset) % PLANES
        floor = PLANES - 1 - offset
        if top < LANES:
            above = jnp.where(lane == top, 0.0, above)
        if 0 <= floor < LANES:
            below = jnp.where(lane == floor, u(j) - ghost(j), below)
        total = (shift_x(u(j), 1) + shift_x(u(j), -1)) + (below + above)
        total = total + (flat_shift(memo, "u", u, lane, j, PLANES) + flat_shift(memo, "u", u, lane, j, -PLANES))
        total = (total - 6.0 * u(j))[:rows]
        centre = u(j)[:rows]
        new = (centre + centre) - at(old, j)[:rows] + (H2 * at(mod, j)[:rows]) * total
        if last:
            dst[:, pl.ds(dst_pad + j * LANES, LANES)] = new
        else:
            dst[:, lanes_of(base + j)] = new


def floor_lane(tile):
    if tile % PERIOD == 0:
        return None
    return (tile - 1) // PERIOD, 16 * ((tile - 1) % PERIOD) + 15


def exact_dot(a, b):
    return jnp.dot(a, b, precision=lax.Precision.HIGHEST, preferred_element_type=jnp.float32)


def kernel(
    sizes, own_tiles, cur_hbm, prev_hbm, mat_hbm, prior_hbm, fields_ref, floor_ref,
    cur, prev, mat, p1, p2, p3, d0, d1, d2, d3, d4, before, stiff, sz, sx, ex, ez, lap,
    prior, deep, packed, arrived, spread, moved, returned,
    load_sem, send_sem, recv_sem, deep_send, deep_recv, trace_send, trace_recv, move_send, move_recv,
):
    half, gx, gy = lax.axis_index("half"), lax.axis_index("gx"), lax.axis_index("gy")
    n_x, n_y = sizes
    wet = half == 0
    groups = own_tiles // PERIOD

    def exists(dx, dy):
        x, y = gx + dx, gy + dy
        return (x >= 0) & (x < n_x) & (y >= 0) & (y < n_y)

    loads = [
        pltpu.make_async_copy(src.at[0], dst.at[0:8, lanes_of(0, own_tiles)], load_sem.at[n])
        for n, (src, dst) in enumerate(((cur_hbm, cur), (prev_hbm, prev), (mat_hbm, mat)))
    ]
    loads.append(pltpu.make_async_copy(prior_hbm, prior, load_sem.at[3]))
    for copy in loads:
        copy.start()

    barrier = pltpu.get_barrier_semaphore()
    count = jnp.int32(1)
    for dx, dy in DIRS:
        here = exists(dx, dy)
        count = count + here.astype(jnp.int32)

        @pl.when(here)
        def _(dx=dx, dy=dy):
            pl.semaphore_signal(barrier, inc=1, device_id={"gx": gx + dx, "gy": gy + dy}, device_id_type=MESH)

    pl.semaphore_signal(barrier, inc=1, device_id={"half": 1 - half}, device_id_type=MESH)

    def halo_copies(dx, dy):
        out = []
        for n, (ref, depth) in enumerate(((cur, STEPS), (prev, STEPS - 1), (mat, STEPS - 1))):
            width = -(-depth * PLANES // LANES)
            if dy == 0:
                src_lanes = dst_lanes = lanes_of(0, own_tiles)
            elif dy == 1:
                src_lanes, dst_lanes = lanes_of(own_tiles - width, width), lanes_of(-width, width)
            else:
                src_lanes, dst_lanes = lanes_of(0, width), lanes_of(own_tiles, width)
            slot = DIRS.index((dx, dy)) * 3 + n
            out.append(
                pltpu.make_async_remote_copy(
                    src_ref=ref.at[rows_sent(dx, depth), src_lanes],
                    dst_ref=ref.at[rows_landed(dx, depth), dst_lanes],
                    send_sem=send_sem.at[slot],
                    recv_sem=recv_sem.at[slot],
                    device_id={"gx": gx + dx, "gy": gy + dy},
                    device_id_type=MESH,
                )
            )
        return out

    def deep_lanes(dy, landed):
        if dy == 0:
            return pl.ds(LANES, groups * LANES)
        if landed:
            return pl.ds(0 if dy == 1 else (groups + 1) * LANES, LANES)
        return pl.ds((groups if dy == 1 else 1) * LANES, LANES)

    def deep_copy(dx, dy):
        slot = DIRS.index((dx, dy))
        return pltpu.make_async_remote_copy(
            src_ref=deep.at[rows_sent(dx, STEPS), deep_lanes(dy, False)],
            dst_ref=deep.at[rows_landed(dx, STEPS), deep_lanes(dy, True)],
            send_sem=deep_send.at[slot],
            recv_sem=deep_recv.at[slot],
            device_id={"gx": gx + dx, "gy": gy + dy},
            device_id_type=MESH,
        )

    for dx, dy in DIRS:
        @pl.when(jnp.logical_not(exists(-dx, -dy)))
        def _(dx=dx, dy=dy):
            lanes = {0: lanes_of(0, own_tiles), 1: lanes_of(-5, 5), -1: lanes_of(own_tiles, 5)}[dy]
            for ref in (cur, prev, mat):
                ref[rows_landed(dx, STEPS), lanes] = jnp.zeros((8 if dx == 0 else 4, lanes.size), jnp.float32)
            lanes = deep_lanes(dy, True)
            deep[rows_landed(dx, STEPS), lanes] = jnp.zeros((8 if dx == 0 else STEPS, lanes.size), jnp.float32)

    for copy in loads:
        copy.wait()
    lane = lax.broadcasted_iota(jnp.int32, (ROWS, LANES), 1)
    lane8 = lane[:8]
    within = lane8 % 16

    @pl.when(wet)
    def _():
        cells = 8 * groups
        row = lax.broadcasted_iota(jnp.int32, (cells, groups * LANES), 0)
        col = lax.broadcasted_iota(jnp.int32, (cells, groups * LANES), 1)
        place = (col == LANES * (row // 8) + 16 * (row % 8) + 15).astype(jnp.float32)
        wave = exact_dot(jnp.concatenate([prior[t] for t in range(STEPS)], 0), place)
        spread[STEPS - 1, 0:8, pl.ds(LANES, groups * LANES)] = wave[8 * (STEPS - 1) :]

        for g in range(groups):
            tile = jnp.zeros((8, LANES), jnp.float32)
            for n, (ref, depth) in enumerate(((cur, STEPS), (prev, STEPS - 1), (mat, STEPS - 1))):
                planes = None
                for j in range(8):
                    value = ref[0:8, lanes_of(g * PERIOD + j + 1)]
                    planes = value if planes is None else jnp.where(lane8 // 16 == j, value, planes)
                tile = tile + turn(jnp.where(within >= 16 - depth, planes, 0.0), 4 * n)
            for t in range(STEPS - 1):
                tile = tile + turn(wave[8 * t : 8 * t + 8, g * LANES : (g + 1) * LANES], 15 - t)
            deep[0:8, pl.ds((g + 1) * LANES, LANES)] = tile

    pl.semaphore_wait(barrier, count)

    order = sorted(DIRS, key=lambda d: (d[1] == 0, d[0] != 0))
    for dx, dy in order:
        @pl.when(exists(dx, dy) & wet)
        def _(dx=dx, dy=dy):
            deep_copy(dx, dy).start()

    for dx, dy in order:
        @pl.when(exists(dx, dy))
        def _(dx=dx, dy=dy):
            for copy in halo_copies(dx, dy):
                copy.start()

    def await_rim(dx, dy):
        @pl.when(exists(-dx, -dy))
        def _():
            for copy in halo_copies(dx, dy):
                copy.wait_recv()

    levels = (cur, p1, p2, p3)
    olds = (prev, cur, p1, p2)
    width = own_tiles * LANES

    def over_tiles(block, t):
        edge = -(-(STEPS - 1 - t) * PLANES // LANES)
        block(range(-edge, own_tiles + edge))

    def trace_copy(t):
        return pltpu.make_async_remote_copy(
            src_ref=packed.at[t], dst_ref=arrived.at[t], send_sem=trace_send.at[t], recv_sem=trace_recv.at[t],
            device_id={"half": 1 - half}, device_id_type=MESH,
        )

    def move_copy(t):
        return pltpu.make_async_remote_copy(
            src_ref=moved.at[t], dst_ref=returned.at[t], send_sem=move_send.at[t], recv_sem=move_recv.at[t],
            device_id={"half": 1 - half}, device_id_type=MESH,
        )

    def dense(value, first):
        cells = 8 * groups
        row = lax.broadcasted_iota(jnp.int32, (LANES, cells), 0)
        col = lax.broadcasted_iota(jnp.int32, (LANES, cells), 1)
        pick = (row == 16 * (col % 8) + first + col // 8).astype(jnp.float32)
        return exact_dot(value, pick)

    @pl.when(wet)
    def _():
        for dx, dy in DIRS:
            @pl.when(exists(-dx, -dy))
            def _(dx=dx, dy=dy):
                deep_copy(dx, dy).wait_recv()

        blocks = range(-1, groups + 1)
        floor_lanes = lane % 16 == 15

        def send_trace(t, tiles):
            total = None
            for g in blocks:
                tile = turn(jnp.where(floor_lanes, tiles[g], 0.0), 15 - (g + 1))
                total = tile if total is None else total + tile
            packed[t] = total
            trace_copy(t).start()

        def ghost_tile(t, g):
            return spread[t, :, pl.ds((g + 1) * LANES, LANES)]

        now = {g: deep[:, pl.ds((g + 1) * LANES, LANES)] for g in blocks}
        send_trace(0, now)
        then = {g: turn(now[g], -4) for g in blocks}
        speed = {g: turn(now[g], -8) for g in blocks}
        for t in range(STEPS - 1):
            for g in blocks:
                spread[t, :, pl.ds((g + 1) * LANES, LANES)] = turn(now[g], t - 15)
        for t in range(STEPS - 1):
            memo = Tiles()
            later = {}
            inside = {g: now[g] for g in blocks}
            inside[-2] = inside[groups + 1] = jnp.zeros((ROWS, LANES), jnp.float32)

            def of(g, inside=inside):
                return inside[g]

            for g in blocks:
                u = now[g]
                below = jnp.where(floor_lanes, u - ghost_tile(t, g), turn(u, 1))
                total = (shift_x(u, 1) + shift_x(u, -1)) + (below + turn(u, -1))
                total = total + (
                    flat_shift(memo, "u", of, lane, g, 16) + flat_shift(memo, "u", of, lane, g, -16)
                )
                later[g] = (u + u) - then[g] + (H2 * speed[g]) * (total - 6.0 * u)
            then, now = now, later
            send_trace(t + 1, now)

        for dx, dy in DIRS:
            await_rim(dx, dy)

        for t in range(STEPS):
            src, old = levels[t], olds[t]
            last = t == STEPS - 1

            def block(tiles, t=t, src=src, old=old, last=last):
                def ghost(j):
                    return ghost_tile(t, (j - 1) // PERIOD)

                dst = fields_ref.at[0] if last else levels[t + 1]
                water_block(src, old, dst, mat, ghost, 0, 0, tiles, last)

            over_tiles(block, t)

        for t in range(STEPS):
            move_copy(t).wait_recv()
            motion = jnp.where(lane[:8] < HALVES, returned[t], turn(returned[t], THICK - HALVES))
            floor_ref[0, t] = RELAXATION * motion[:, : 8 * groups] + (1.0 - RELAXATION) * prior[t]
            trace_copy(t).wait_send()

    @pl.when(jnp.logical_not(wet))
    def _():
        def convert(rows, slots, base=0, shift=0):
            def put(ref):
                def store(slot, parts):
                    for c in range(3):
                        ref[slot + shift, c, rows] = parts[c]
                return store

            def put_stiff(slot, parts):
                light = H2 * parts[2]
                stiff[slot + shift, 0, rows] = light * parts[0]
                stiff[slot + shift, 1, rows] = light * parts[1]
                stiff[slot + shift, 2, rows] = light

            inner = [slot for slot in slots if 0 < slot < SLOTS - 1]
            to_planes(cur, rows, slots, base, put(d0))
            to_planes(prev, rows, inner, base, put(before))
            to_planes(mat, rows, inner, base, put_stiff)

        def convert_inner(rows):
            @pl.loop(0, HALVES // 8)
            def _(n):
                convert(rows, range(STEPS, STEPS + 8), n * PERIOD, n * 8)

        upper, lower = pl.ds(0, 8), pl.ds(8, 8)
        convert_inner(upper)
        for dx, dy in DIRS:
            if dy == 0:
                await_rim(dx, dy)
        convert_inner(lower)
        for dx, dy in DIRS:
            if dy != 0:
                await_rim(dx, dy)
        for rows in (upper, lower):
            convert(rows, (*range(STEPS), *range(SLOTS - STEPS, SLOTS)))

        displaced = (d0, d1, d2, d3, d4)
        earlier = (before, d0, d1, d2)
        scratch = (sz, sx, ex, ez, lap)
        for t in range(STEPS):
            last = t == STEPS - 1
            rows = 8 if last else ROWS
            src, old, dst = displaced[t], earlier[t], displaced[t + 1]

            for slot in range(t, SLOTS - t):
                slopes(src, t, slot, *scratch, rows)

            trace_copy(t).wait_recv()
            load = arrived[t][:rows]
            lane_out = lane[:rows]

            def pushed(slot, load=load, lane_out=lane_out):
                cell = slot - STEPS
                near = cell % 8 * 16 + 1 + cell // 8
                return jnp.where(
                    lane_out == 0, turn(load, near),
                    jnp.where(lane_out == THICK, turn(load, near + HALVES // 8 - THICK), 0.0),
                )

            total = jnp.zeros((8, LANES), jnp.float32)
            for slot in range(t + 1, SLOTS - 1 - t):
                acc = advance_slot(src, old, dst, t, slot, *scratch, stiff, pushed(slot), rows)
                cell = slot - STEPS
                if 0 <= cell < HALVES:
                    total = jnp.where((lane8 == cell) | (lane8 == THICK + cell), turn(acc[:8], -cell), total)
            moved[t] = total * (1.0 / H2)
            move_copy(t).start()

        from_planes(d4, fields_ref.at[0], range(own_tiles))
        for t in range(STEPS):
            floor_ref[0, t] = dense(arrived[t, 0:8], 1)
            move_copy(t).wait_send()

    for dx, dy in DIRS:
        @pl.when(exists(dx, dy))
        def _(dx=dx, dy=dy):
            for copy in halo_copies(dx, dy):
                copy.wait_send()

            @pl.when(wet)
            def _():
                deep_copy(dx, dy).wait_send()


def deliver(fields_ref, floor_ref, fields_out, floor_out, sem):
    copies = [
        pltpu.make_async_copy(src, dst, sem.at[n])
        for n, (src, dst) in enumerate(((fields_ref, fields_out), (floor_ref, floor_out)))
    ]
    for copy in copies:
        copy.start()
    for copy in copies:
        copy.wait()


def on_device(sizes, current, previous, material, prior):
    own = current.shape[2]
    own_tiles = own // LANES
    groups = own_tiles // PERIOD
    cells = own // PLANES
    field = pltpu.VMEM((ROWS, (own_tiles + 2 * PAD) * LANES), jnp.float32)
    planes = pltpu.VMEM((SLOTS, 3, ROWS, LANES), jnp.float32)

    def per_level(count):
        return pltpu.VMEM((STEPS, SLOTS) + count + (ROWS, LANES), jnp.float32)

    anywhere = pl.BlockSpec(memory_space=pl.ANY)
    near = pl.BlockSpec(memory_space=pltpu.VMEM)
    dma = pltpu.SemaphoreType.DMA
    held = pl.pallas_call(
        functools.partial(kernel, sizes, own_tiles),
        out_shape=(
            pltpu.VMEM(current.shape, jnp.float32),
            pltpu.VMEM((1,) + prior.shape, jnp.float32),
        ),
        in_specs=[anywhere] * 4,
        out_specs=(near, near),
        scratch_shapes=[field] * 6
        + [planes] * 7
        + [per_level((2,)), per_level((2,)), per_level(()), per_level(()), per_level((3,))]
        + [
            pltpu.VMEM(prior.shape, jnp.float32),
            pltpu.VMEM((ROWS, (groups + 2) * LANES), jnp.float32),
            pltpu.VMEM((STEPS, ROWS, LANES), jnp.float32),
            pltpu.VMEM((STEPS, ROWS, LANES), jnp.float32),
            pltpu.VMEM((STEPS, ROWS, (groups + 2) * LANES), jnp.float32),
            pltpu.VMEM((STEPS, 8, LANES), jnp.float32),
            pltpu.VMEM((STEPS, 8, LANES), jnp.float32),
            dma((4,)),
            dma((3 * len(DIRS),)),
            dma((3 * len(DIRS),)),
            dma((len(DIRS),)),
            dma((len(DIRS),)),
            dma((STEPS,)),
            dma((STEPS,)),
            dma((STEPS,)),
            dma((STEPS,)),
        ],
        compiler_params=pltpu.CompilerParams(collective_id=0, has_side_effects=True),
    )(current, previous, material, prior)
    return pl.pallas_call(
        deliver,
        out_shape=tuple(jax.ShapeDtypeStruct(x.shape, x.dtype) for x in held),
        in_specs=[near] * 2,
        out_specs=(anywhere, anywhere),
        scratch_shapes=[dma((2,))],
    )(*(pltpu.with_memory_space_constraint(x, pltpu.VMEM) for x in held))


def solution(mesh):
    placed = (
        P("half", "gx", "gy"),
        P("half", "gx", "gy"),
        P("half", "gx", "gy"),
        P(None, "gx", "gy"),
    )
    return jax.shard_map(
        functools.partial(on_device, (mesh.shape["gx"], mesh.shape["gy"])),
        mesh=mesh,
        in_specs=placed,
        out_specs=(P("half", "gx", "gy"), P("half", None, "gx", "gy")),
        check_vma=False,
    )
```

```python
import functools

import jax
import jax.numpy as jnp
from jax import lax
from jax.experimental import pallas as pl
from jax.experimental.pallas import tpu as pltpu
from jax.sharding import PartitionSpec as P

STEPS = 4
PLANES = 144
THICK = PLANES // 3
TIME_STEP = 0.22
RELAXATION = 0.5
H2 = TIME_STEP * TIME_STEP

LANES = 128
ROWS = 16
PAD = 8
HALVES = 16
SLOTS = HALVES + 2 * STEPS
PERIOD = 9
MESH = pl.DeviceIdType.MESH
DIRS = tuple((dx, dy) for dx in (-1, 0, 1) for dy in (-1, 0, 1) if (dx, dy) != (0, 0))


def lanes_of(tile, count=1):
    start = (tile + PAD) * LANES
    if not isinstance(start, int):
        start = pl.multiple_of(start, LANES)
    return pl.ds(start, count * LANES)


def rows_sent(dx, depth):
    return {0: pl.ds(0, 8), 1: pl.ds(8 - depth, depth), -1: pl.ds(0, depth)}[dx]


def rows_landed(dx, depth):
    return {0: pl.ds(0, 8), 1: pl.ds(16 - depth, depth), -1: pl.ds(8, depth)}[dx]


def shift_x(value, by):
    return pltpu.roll(value, (-by) % ROWS, 0)


def turn(value, by):
    return pltpu.roll(value, (-by) % LANES, 1)


class Tiles:
    def __init__(self):
        self.known = {}

    def get(self, name, tile, make):
        key = (name, tile)
        if key not in self.known:
            self.known[key] = make()
        return self.known[key]


def flat_shift(memo, name, of, lane, tile, by):
    whole, part = divmod(by, LANES)
    first = memo.get(("turn", name, part), tile + whole, lambda: turn(of(tile + whole), part))
    if part == 0:
        return first
    second = memo.get(("turn", name, part), tile + whole + 1, lambda: turn(of(tile + whole + 1), part))
    return jnp.where(lane < LANES - part, first, second)


def unit_window(memo, of, lane, start, low, high):
    tile, part = divmod(start, LANES)
    if part + low >= LANES:
        tile, part, low, high = tile + 1, part - LANES, low, high
    first = memo.get("turn", (tile, part % LANES), lambda: turn(of(tile), part % LANES))
    if part + high <= LANES:
        return first
    second = memo.get("turn", (tile + 1, part % LANES), lambda: turn(of(tile + 1), part % LANES))
    return jnp.where(lane < LANES - part, first, second)


def to_planes(ref, rows, slots, base, store):
    memo = Tiles()
    lane = lax.broadcasted_iota(jnp.int32, (8, LANES), 1)

    def of(tile):
        return memo.get("load", tile, lambda: ref[rows, lanes_of(base + tile)])

    for slot in slots:
        parts = []
        for c in range(3):
            near = (slot - STEPS) * PLANES + c * THICK
            far = near + HALVES * PLANES - THICK
            parts.append(
                jnp.where(
                    lane < THICK,
                    unit_window(memo, of, lane, near, 0, THICK),
                    unit_window(memo, of, lane, far, THICK, 2 * THICK),
                )
            )
        store(slot, parts)


def from_planes(planes, dst, tiles):
    lane = lax.broadcasted_iota(jnp.int32, (8, LANES), 1)
    for q in tiles:
        out = None
        for n in range(q * LANES // THICK, (q * LANES + LANES - 1) // THICK + 1):
            cell, c = divmod(n, 3)
            far = cell >= HALVES
            slot = cell + STEPS - (HALVES if far else 0)
            value = turn(planes[slot, c, 0:8], q * LANES - n * THICK + (THICK if far else 0))
            out = value if out is None else jnp.where(lane < n * THICK - q * LANES, out, value)
        dst[:, pl.ds(q * LANES, LANES)] = out


def slopes(src, level, slot, sz, sx, ex, ez, lap, rows):
    lane = lax.broadcasted_iota(jnp.int32, (ROWS, LANES), 1)
    keep_up = jnp.where((lane == THICK - 1) | (lane >= 2 * THICK - 1), 0.0, 1.0)
    keep_down = jnp.where((lane == 0) | (lane == THICK), 0.0, 1.0)
    lap_x, lap_z, mixed = [], [], []
    for c in range(3):
        u = src[slot, c]
        up, down = turn(u, 1) * keep_up, turn(u, -1) * keep_down
        right, left = shift_x(u, 1)[:rows], shift_x(u, -1)[:rows]
        slope_z = (up - down) * 0.25
        lap_z.append((up + down)[:rows])
        lap_x.append(right + left)
        if c < 2:
            sx[level, slot, c, 0:rows] = (right - left) * 0.25
        if c > 0:
            sz[level, slot, c - 1, 0:rows] = slope_z[:rows]
        if c != 1:
            mixed.append((shift_x(slope_z, 1) - shift_x(slope_z, -1))[:rows])
        lap[level, slot, c, 0:rows] = lap_x[c] + lap_z[c]
    ex[level, slot, 0:rows] = lap_x[0] + mixed[1]
    ez[level, slot, 0:rows] = lap_z[2] + mixed[0]


def advance_slot(src, old, dst, level, slot, sz, sx, ex, ez, lap, stiff, pushed, rows):
    bulk, shear, light = (stiff[slot, n, 0:rows] for n in range(3))
    centre = [src[slot, c, 0:rows] for c in range(3)]
    lap_y = [src[slot + 1, c, 0:rows] + src[slot - 1, c, 0:rows] for c in range(3)]

    def along(ref, c):
        return ref[level, slot + 1, c, 0:rows] - ref[level, slot - 1, c, 0:rows]

    grad = (
        ex[level, slot, 0:rows] + along(sx, 1),
        lap_y[1] + (along(sx, 0) + along(sz, 1)),
        ez[level, slot, 0:rows] + along(sz, 0),
    )
    for c in range(3):
        twice = centre[c] + centre[c]
        total = lap[level, slot, c, 0:rows] + lap_y[c] - 6.0 * centre[c]
        acc = bulk * (grad[c] - twice) + shear * total
        if c == 2:
            acc = acc + light * pushed
        dst[slot, c, 0:rows] = twice - old[slot, c, 0:rows] + acc
    return acc


def water_block(src, old, dst, mod, ghost, dst_pad, base, tiles, last):
    memo = Tiles()
    lane = lax.broadcasted_iota(jnp.int32, (ROWS, LANES), 1)
    rows = 8 if last else ROWS

    def at(ref, j):
        return ref[:, lanes_of(base + j)]

    def u(j):
        return memo.get("u", j, lambda: at(src, j))

    for j in tiles:
        below = flat_shift(memo, "u", u, lane, j, 1)
        above = flat_shift(memo, "u", u, lane, j, -1)
        offset = (j * LANES) % PLANES
        top = (-offset) % PLANES
        floor = PLANES - 1 - offset
        if top < LANES:
            above = jnp.where(lane == top, 0.0, above)
        if 0 <= floor < LANES:
            below = jnp.where(lane == floor, u(j) - ghost(j), below)
        total = (shift_x(u(j), 1) + shift_x(u(j), -1)) + (below + above)
        total = total + (flat_shift(memo, "u", u, lane, j, PLANES) + flat_shift(memo, "u", u, lane, j, -PLANES))
        total = (total - 6.0 * u(j))[:rows]
        centre = u(j)[:rows]
        new = (centre + centre) - at(old, j)[:rows] + (H2 * at(mod, j)[:rows]) * total
        if last:
            dst[:, pl.ds(dst_pad + j * LANES, LANES)] = new
        else:
            dst[:, lanes_of(base + j)] = new


def top_slopes(src, c, g, at, sz, sx, ex, lap, rows):
    lane = lax.broadcasted_iota(jnp.int32, (ROWS, LANES), 1)
    u = src[c, :, at(g)]
    up, down = turn(u, 1), jnp.where(lane % 16 == 0, 0.0, turn(u, -1))
    right, left = shift_x(u, 1)[:rows], shift_x(u, -1)[:rows]
    slope = (up - down) * 0.25
    sz[c, 0:rows, at(g)] = slope[:rows]
    sx[c, 0:rows, at(g)] = (right - left) * 0.25
    lap_x, lap_z = right + left, (up + down)[:rows]
    lap[c, 0:rows, at(g)] = lap_x + lap_z
    mixed = (shift_x(slope, 1) - shift_x(slope, -1))[:rows]
    ex[c, 0:rows, at(g)] = mixed
    return lap_x, lap_z


def top_update(src, old, dst, g, at, sz, sx, ex, self_terms, lap, stiff, pushed, rows):
    lane = lax.broadcasted_iota(jnp.int32, (rows, LANES), 1)
    memo = Tiles()

    def along(name, ref, c, by):
        return flat_shift(memo, (name, c), lambda n: ref[c, 0:rows, at(n)], lane, g, by)

    def cross(name, ref, c):
        return along(name, ref, c, 16) - along(name, ref, c, -16)

    bulk, shear, light = (stiff[n, 0:rows, at(g)] for n in range(3))
    acc = None
    for c in range(3):
        if dst is None and c < 2:
            continue
        u = src[c, 0:rows, at(g)]
        lap_y = along("u", src, c, 16) + along("u", src, c, -16)
        if c == 0:
            grad = self_terms[0, 0:rows, at(g)] + (cross("sx", sx, 1) + ex[2, 0:rows, at(g)])
        elif c == 1:
            grad = lap_y + (cross("sx", sx, 0) + cross("sz", sz, 2))
        else:
            grad = self_terms[1, 0:rows, at(g)] + (ex[0, 0:rows, at(g)] + cross("sz", sz, 1))
        twice = u + u
        total = lap[c, 0:rows, at(g)] + lap_y - 6.0 * u
        acc = bulk * (grad - twice) + shear * total
        if c == 2:
            acc = acc + light * pushed
        if dst is not None:
            dst[c, 0:rows, at(g)] = twice - old[c, 0:rows, at(g)] + acc
    return acc


def floor_lane(tile):
    if tile % PERIOD == 0:
        return None
    return (tile - 1) // PERIOD, 16 * ((tile - 1) % PERIOD) + 15


def exact_dot(a, b):
    return jnp.dot(a, b, precision=lax.Precision.HIGHEST, preferred_element_type=jnp.float32)


def kernel(
    sizes, own_tiles, cur_hbm, prev_hbm, mat_hbm, prior_hbm, fields_ref, floor_ref,
    cur, prev, mat, p1, p2, p3, d0, d1, d2, d3, d4, before, stiff, sz, sx, ex, ez, lap,
    prior, deep, packed, arrived, spread, crown, samples, t0, t1, t2, t3, told, tstiff, tsz, tsx, tex, tself, tlap,
    load_sem, send_sem, recv_sem, deep_send, deep_recv, trace_send, trace_recv, crown_send, crown_recv,
):
    half, gx, gy = lax.axis_index("half"), lax.axis_index("gx"), lax.axis_index("gy")
    n_x, n_y = sizes
    wet = half == 0
    groups = own_tiles // PERIOD

    def exists(dx, dy):
        x, y = gx + dx, gy + dy
        return (x >= 0) & (x < n_x) & (y >= 0) & (y < n_y)

    loads = [
        pltpu.make_async_copy(src.at[0], dst.at[0:8, lanes_of(0, own_tiles)], load_sem.at[n])
        for n, (src, dst) in enumerate(((cur_hbm, cur), (prev_hbm, prev), (mat_hbm, mat)))
    ]
    loads.append(pltpu.make_async_copy(prior_hbm, prior, load_sem.at[3]))
    for copy in loads:
        copy.start()

    barrier = pltpu.get_barrier_semaphore()
    count = jnp.int32(1)
    for dx, dy in DIRS:
        here = exists(dx, dy)
        count = count + 2 * here.astype(jnp.int32)

        @pl.when(here)
        def _(dx=dx, dy=dy):
            for medium in (half, 1 - half):
                there = {"half": medium, "gx": gx + dx, "gy": gy + dy}
                pl.semaphore_signal(barrier, inc=1, device_id=there, device_id_type=MESH)

    pl.semaphore_signal(barrier, inc=1, device_id={"half": 1 - half}, device_id_type=MESH)

    def halo_copies(dx, dy):
        out = []
        for n, (ref, depth) in enumerate(((cur, STEPS), (prev, STEPS - 1), (mat, STEPS - 1))):
            width = -(-depth * PLANES // LANES)
            if dy == 0:
                src_lanes = dst_lanes = lanes_of(0, own_tiles)
            elif dy == 1:
                src_lanes, dst_lanes = lanes_of(own_tiles - width, width), lanes_of(-width, width)
            else:
                src_lanes, dst_lanes = lanes_of(0, width), lanes_of(own_tiles, width)
            slot = DIRS.index((dx, dy)) * 3 + n
            out.append(
                pltpu.make_async_remote_copy(
                    src_ref=ref.at[rows_sent(dx, depth), src_lanes],
                    dst_ref=ref.at[rows_landed(dx, depth), dst_lanes],
                    send_sem=send_sem.at[slot],
                    recv_sem=recv_sem.at[slot],
                    device_id={"gx": gx + dx, "gy": gy + dy},
                    device_id_type=MESH,
                )
            )
        return out

    def deep_lanes(dy, landed):
        if dy == 0:
            return pl.ds(LANES, groups * LANES)
        if landed:
            return pl.ds(0 if dy == 1 else (groups + 1) * LANES, LANES)
        return pl.ds((groups if dy == 1 else 1) * LANES, LANES)

    def deep_copy(dx, dy):
        slot = DIRS.index((dx, dy))
        return pltpu.make_async_remote_copy(
            src_ref=deep.at[rows_sent(dx, STEPS), deep_lanes(dy, False)],
            dst_ref=deep.at[rows_landed(dx, STEPS), deep_lanes(dy, True)],
            send_sem=deep_send.at[slot],
            recv_sem=deep_recv.at[slot],
            device_id={"gx": gx + dx, "gy": gy + dy},
            device_id_type=MESH,
        )

    def crown_copy(dx, dy):
        slot = DIRS.index((dx, dy))
        return pltpu.make_async_remote_copy(
            src_ref=crown.at[:, rows_sent(dx, STEPS), deep_lanes(dy, False)],
            dst_ref=crown.at[:, rows_landed(dx, STEPS), deep_lanes(dy, True)],
            send_sem=crown_send.at[slot],
            recv_sem=crown_recv.at[slot],
            device_id={"half": 1 - half, "gx": gx + dx, "gy": gy + dy},
            device_id_type=MESH,
        )

    def crown_up():
        own = crown.at[:, 0:8, deep_lanes(0, False)]
        return pltpu.make_async_remote_copy(
            src_ref=own, dst_ref=own, send_sem=crown_send.at[len(DIRS)], recv_sem=crown_recv.at[len(DIRS)],
            device_id={"half": 1 - half}, device_id_type=MESH,
        )

    for dx, dy in DIRS:
        @pl.when(jnp.logical_not(exists(-dx, -dy)))
        def _(dx=dx, dy=dy):
            lanes = {0: lanes_of(0, own_tiles), 1: lanes_of(-5, 5), -1: lanes_of(own_tiles, 5)}[dy]
            for ref in (cur, prev, mat):
                ref[rows_landed(dx, STEPS), lanes] = jnp.zeros((8 if dx == 0 else 4, lanes.size), jnp.float32)
            lanes = deep_lanes(dy, True)
            blank = jnp.zeros((8 if dx == 0 else STEPS, lanes.size), jnp.float32)
            deep[rows_landed(dx, STEPS), lanes] = blank
            for c in range(3):
                crown[c, rows_landed(dx, STEPS), lanes] = blank

    for copy in loads:
        copy.wait()
    lane = lax.broadcasted_iota(jnp.int32, (ROWS, LANES), 1)
    lane8 = lane[:8]
    within = lane8 % 16

    @pl.when(wet)
    def _():
        cells = 8 * groups
        row = lax.broadcasted_iota(jnp.int32, (cells, groups * LANES), 0)
        col = lax.broadcasted_iota(jnp.int32, (cells, groups * LANES), 1)
        place = (col == LANES * (row // 8) + 16 * (row % 8) + 15).astype(jnp.float32)
        wave = exact_dot(jnp.concatenate([prior[t] for t in range(STEPS)], 0), place)
        spread[STEPS - 1, 0:8, pl.ds(LANES, groups * LANES)] = wave[8 * (STEPS - 1) :]

        for g in range(groups):
            tile = jnp.zeros((8, LANES), jnp.float32)
            for n, (ref, depth) in enumerate(((cur, STEPS), (prev, STEPS - 1), (mat, STEPS - 1))):
                planes = None
                for j in range(8):
                    value = ref[0:8, lanes_of(g * PERIOD + j + 1)]
                    planes = value if planes is None else jnp.where(lane8 // 16 == j, value, planes)
                tile = tile + turn(jnp.where(within >= 16 - depth, planes, 0.0), 4 * n)
            for t in range(STEPS - 1):
                tile = tile + turn(wave[8 * t : 8 * t + 8, g * LANES : (g + 1) * LANES], 15 - t)
            deep[0:8, pl.ds((g + 1) * LANES, LANES)] = tile

    @pl.when(jnp.logical_not(wet))
    def _():
        for g in range(groups):
            for c in range(3):
                tile = None
                for ref, depth, lead in ((cur, 5, 0), (prev, 4, 5), (mat, 4, 9)):
                    planes = None
                    for j in range(8):
                        q = g * PERIOD + (PLANES * j + THICK * c) // LANES
                        spot = (j + 3 * c) % 8
                        value = ref[0:8, lanes_of(q)]
                        planes = value if planes is None else jnp.where(lane8 // 16 == spot, value, planes)
                    part = jnp.where(within < depth, planes, 0.0)
                    if (THICK * c - lead) % LANES:
                        part = turn(part, THICK * c - lead)
                    tile = part if tile is None else tile + part
                crown[c, 0:8, pl.ds((g + 1) * LANES, LANES)] = tile

    pl.semaphore_wait(barrier, count)


    order = sorted(DIRS, key=lambda d: (d[1] == 0, d[0] != 0))
    for dx, dy in order:
        @pl.when(exists(dx, dy) & wet)
        def _(dx=dx, dy=dy):
            deep_copy(dx, dy).start()

        @pl.when(exists(dx, dy) & jnp.logical_not(wet))
        def _(dx=dx, dy=dy):
            crown_copy(dx, dy).start()

    @pl.when(jnp.logical_not(wet))
    def _():
        crown_up().start()

    for dx, dy in order:
        @pl.when(exists(dx, dy))
        def _(dx=dx, dy=dy):
            for copy in halo_copies(dx, dy):
                copy.start()

    def await_rim(dx, dy):
        @pl.when(exists(-dx, -dy))
        def _():
            for copy in halo_copies(dx, dy):
                copy.wait_recv()

    levels = (cur, p1, p2, p3)
    olds = (prev, cur, p1, p2)
    width = own_tiles * LANES

    def over_tiles(block, t):
        edge = -(-(STEPS - 1 - t) * PLANES // LANES)
        block(range(-edge, own_tiles + edge))

    def trace_copy(t):
        return pltpu.make_async_remote_copy(
            src_ref=packed.at[t], dst_ref=arrived.at[t], send_sem=trace_send.at[t], recv_sem=trace_recv.at[t],
            device_id={"half": 1 - half}, device_id_type=MESH,
        )

    def dense(value, first):
        cells = 8 * groups
        row = lax.broadcasted_iota(jnp.int32, (LANES, cells), 0)
        col = lax.broadcasted_iota(jnp.int32, (LANES, cells), 1)
        pick = (row == 16 * (col % 8) + first + col // 8).astype(jnp.float32)
        return exact_dot(value, pick)

    @pl.when(wet)
    def _():
        for dx, dy in DIRS:
            @pl.when(exists(-dx, -dy))
            def _(dx=dx, dy=dy):
                deep_copy(dx, dy).wait_recv()

        blocks = range(-1, groups + 1)
        floor_lanes = lane % 16 == 15

        def send_trace(t, tiles):
            for g in blocks:
                samples[t, :, pl.ds((g + 1) * LANES, LANES)] = jnp.where(lane % 16 == 0, turn(tiles[g], 15), 0.0)
            total = None
            for g in blocks:
                tile = turn(jnp.where(floor_lanes, tiles[g], 0.0), 15 - (g + 1))
                total = tile if total is None else total + tile
            packed[t] = total
            trace_copy(t).start()

        def ghost_tile(t, g):
            return spread[t, :, pl.ds((g + 1) * LANES, LANES)]

        now = {g: deep[:, pl.ds((g + 1) * LANES, LANES)] for g in blocks}
        send_trace(0, now)
        then = {g: turn(now[g], -4) for g in blocks}
        speed = {g: turn(now[g], -8) for g in blocks}
        for t in range(STEPS - 1):
            for g in blocks:
                spread[t, :, pl.ds((g + 1) * LANES, LANES)] = turn(now[g], t - 15)
        for t in range(STEPS - 1):
            memo = Tiles()
            later = {}
            inside = {g: now[g] for g in blocks}
            inside[-2] = inside[groups + 1] = jnp.zeros((ROWS, LANES), jnp.float32)

            def of(g, inside=inside):
                return inside[g]

            for g in blocks:
                u = now[g]
                below = jnp.where(floor_lanes, u - ghost_tile(t, g), turn(u, 1))
                total = (shift_x(u, 1) + shift_x(u, -1)) + (below + turn(u, -1))
                total = total + (
                    flat_shift(memo, "u", of, lane, g, 16) + flat_shift(memo, "u", of, lane, g, -16)
                )
                later[g] = (u + u) - then[g] + (H2 * speed[g]) * (total - 6.0 * u)
            then, now = now, later
            send_trace(t + 1, now)

        for dx, dy in DIRS:
            @pl.when(exists(-dx, -dy))
            def _(dx=dx, dy=dy):
                crown_copy(dx, dy).wait_recv()

        crown_up().wait_recv()

        def at(g):
            return pl.ds((g + 2) * LANES, LANES)

        first_lanes = lane % 16 == 0
        for ref in (t0, t1, t2, t3, tsz, tsx):
            for c in range(3):
                for g in (-2, groups + 1):
                    ref[c, :, at(g)] = jnp.zeros((ROWS, LANES), jnp.float32)
        for g in blocks:
            tiles = [crown[c, :, pl.ds((g + 1) * LANES, LANES)] for c in range(3)]
            light = H2 * turn(tiles[2], 9)
            tstiff[0, :, at(g)] = light * turn(tiles[0], 9)
            tstiff[1, :, at(g)] = light * turn(tiles[1], 9)
            tstiff[2, :, at(g)] = light
            for c in range(3):
                t0[c, :, at(g)] = tiles[c]
                told[c, :, at(g)] = turn(tiles[c], 5)

        tops, befores = (t0, t1, t2, t3, None), (told, t0, t1, t2)
        for t in range(STEPS):
            last = t == STEPS - 1
            rows = 8 if last else ROWS
            for g in blocks:
                terms = [top_slopes(tops[t], c, g, at, tsz, tsx, tex, tlap, rows) for c in range(3)]
                tself[0, 0:rows, at(g)] = terms[0][0]
                tself[1, 0:rows, at(g)] = terms[2][1]
            total = None
            for g in range(groups) if last else blocks:
                source = samples[t, 0:rows, pl.ds((g + 1) * LANES, LANES)]
                acc = top_update(
                    tops[t], befores[t], tops[t + 1], g, at, tsz, tsx, tex, tself, tlap, tstiff, source, rows
                )
                if 0 <= g < groups:
                    tile = turn(jnp.where(within == 0, acc[:8], 0.0), -g)
                    total = tile if total is None else total + tile
            floor_ref[0, t] = (RELAXATION / H2) * dense(total, 0) + (1.0 - RELAXATION) * prior[t]
            trace_copy(t).wait_send()

        for dx, dy in DIRS:
            await_rim(dx, dy)

        for t in range(STEPS):
            src, old = levels[t], olds[t]
            last = t == STEPS - 1

            def block(tiles, t=t, src=src, old=old, last=last):
                def ghost(j):
                    return ghost_tile(t, (j - 1) // PERIOD)

                dst = fields_ref.at[0] if last else levels[t + 1]
                water_block(src, old, dst, mat, ghost, 0, 0, tiles, last)

            over_tiles(block, t)

    @pl.when(jnp.logical_not(wet))
    def _():
        def convert(rows, slots, base=0, shift=0):
            def put(ref):
                def store(slot, parts):
                    for c in range(3):
                        ref[slot + shift, c, rows] = parts[c]
                return store

            def put_stiff(slot, parts):
                light = H2 * parts[2]
                stiff[slot + shift, 0, rows] = light * parts[0]
                stiff[slot + shift, 1, rows] = light * parts[1]
                stiff[slot + shift, 2, rows] = light

            inner = [slot for slot in slots if 0 < slot < SLOTS - 1]
            to_planes(cur, rows, slots, base, put(d0))
            to_planes(prev, rows, inner, base, put(before))
            to_planes(mat, rows, inner, base, put_stiff)

        def convert_inner(rows):
            @pl.loop(0, HALVES // 8)
            def _(n):
                convert(rows, range(STEPS, STEPS + 8), n * PERIOD, n * 8)

        upper, lower = pl.ds(0, 8), pl.ds(8, 8)
        convert_inner(upper)
        for dx, dy in DIRS:
            if dy == 0:
                await_rim(dx, dy)
        convert_inner(lower)
        for dx, dy in DIRS:
            if dy != 0:
                await_rim(dx, dy)
        for rows in (upper, lower):
            convert(rows, (*range(STEPS), *range(SLOTS - STEPS, SLOTS)))

        displaced = (d0, d1, d2, d3, d4)
        earlier = (before, d0, d1, d2)
        scratch = (sz, sx, ex, ez, lap)
        for t in range(STEPS):
            last = t == STEPS - 1
            rows = 8 if last else ROWS
            src, old, dst = displaced[t], earlier[t], displaced[t + 1]

            for slot in range(t, SLOTS - t):
                slopes(src, t, slot, *scratch, rows)

            trace_copy(t).wait_recv()
            load = arrived[t][:rows]
            lane_out = lane[:rows]

            def pushed(slot, load=load, lane_out=lane_out):
                cell = slot - STEPS
                near = cell % 8 * 16 + 1 + cell // 8
                return jnp.where(
                    lane_out == 0, turn(load, near),
                    jnp.where(lane_out == THICK, turn(load, near + HALVES // 8 - THICK), 0.0),
                )

            for slot in range(t + 1, SLOTS - 1 - t):
                advance_slot(src, old, dst, t, slot, *scratch, stiff, pushed(slot), rows)

        from_planes(d4, fields_ref.at[0], range(own_tiles))
        for t in range(STEPS):
            floor_ref[0, t] = dense(arrived[t, 0:8], 1)
        crown_up().wait_send()

    for dx, dy in DIRS:
        @pl.when(exists(dx, dy))
        def _(dx=dx, dy=dy):
            for copy in halo_copies(dx, dy):
                copy.wait_send()

            @pl.when(wet)
            def _():
                deep_copy(dx, dy).wait_send()

            @pl.when(jnp.logical_not(wet))
            def _():
                crown_copy(dx, dy).wait_send()


def deliver(fields_ref, floor_ref, fields_out, floor_out, sem):
    copies = [
        pltpu.make_async_copy(src, dst, sem.at[n])
        for n, (src, dst) in enumerate(((fields_ref, fields_out), (floor_ref, floor_out)))
    ]
    for copy in copies:
        copy.start()
    for copy in copies:
        copy.wait()


def on_device(sizes, current, previous, material, prior):
    own = current.shape[2]
    own_tiles = own // LANES
    groups = own_tiles // PERIOD
    cells = own // PLANES
    field = pltpu.VMEM((ROWS, (own_tiles + 2 * PAD) * LANES), jnp.float32)
    planes = pltpu.VMEM((SLOTS, 3, ROWS, LANES), jnp.float32)

    def per_level(count):
        return pltpu.VMEM((STEPS, SLOTS) + count + (ROWS, LANES), jnp.float32)

    anywhere = pl.BlockSpec(memory_space=pl.ANY)
    near = pl.BlockSpec(memory_space=pltpu.VMEM)
    dma = pltpu.SemaphoreType.DMA
    held = pl.pallas_call(
        functools.partial(kernel, sizes, own_tiles),
        out_shape=(
            pltpu.VMEM(current.shape, jnp.float32),
            pltpu.VMEM((1,) + prior.shape, jnp.float32),
        ),
        in_specs=[anywhere] * 4,
        out_specs=(near, near),
        scratch_shapes=[field] * 6
        + [planes] * 7
        + [per_level((2,)), per_level((2,)), per_level(()), per_level(()), per_level((3,))]
        + [
            pltpu.VMEM(prior.shape, jnp.float32),
            pltpu.VMEM((ROWS, (groups + 2) * LANES), jnp.float32),
            pltpu.VMEM((STEPS, ROWS, LANES), jnp.float32),
            pltpu.VMEM((STEPS, ROWS, LANES), jnp.float32),
            pltpu.VMEM((STEPS, ROWS, (groups + 2) * LANES), jnp.float32),
            pltpu.VMEM((3, ROWS, (groups + 2) * LANES), jnp.float32),
            pltpu.VMEM((STEPS, ROWS, (groups + 2) * LANES), jnp.float32),
            *[pltpu.VMEM((3, ROWS, (groups + 4) * LANES), jnp.float32)] * 11,
            dma((4,)),
            dma((3 * len(DIRS),)),
            dma((3 * len(DIRS),)),
            dma((len(DIRS),)),
            dma((len(DIRS),)),
            dma((STEPS,)),
            dma((STEPS,)),
            dma((len(DIRS) + 1,)),
            dma((len(DIRS) + 1,)),
        ],
        compiler_params=pltpu.CompilerParams(collective_id=0, has_side_effects=True),
    )(current, previous, material, prior)
    return pl.pallas_call(
        deliver,
        out_shape=tuple(jax.ShapeDtypeStruct(x.shape, x.dtype) for x in held),
        in_specs=[near] * 2,
        out_specs=(anywhere, anywhere),
        scratch_shapes=[dma((2,))],
    )(*(pltpu.with_memory_space_constraint(x, pltpu.VMEM) for x in held))


def solution(mesh):
    placed = (
        P("half", "gx", "gy"),
        P("half", "gx", "gy"),
        P("half", "gx", "gy"),
        P(None, "gx", "gy"),
    )
    return jax.shard_map(
        functools.partial(on_device, (mesh.shape["gx"], mesh.shape["gy"])),
        mesh=mesh,
        in_specs=placed,
        out_specs=(P("half", "gx", "gy"), P("half", None, "gx", "gy")),
        check_vma=False,
    )
```

```python
import functools

import jax
import jax.numpy as jnp
from jax import lax
from jax.experimental import pallas as pl
from jax.experimental.pallas import tpu as pltpu
from jax.sharding import PartitionSpec as P

STEPS = 4
PLANES = 144
THICK = PLANES // 3
TIME_STEP = 0.22
RELAXATION = 0.5
H2 = TIME_STEP * TIME_STEP

LANES = 128
ROWS = 16
PAD = 8
HALVES = 16
SLOTS = HALVES + 2 * STEPS
PERIOD = 9
MESH = pl.DeviceIdType.MESH
DIRS = tuple((dx, dy) for dx in (-1, 0, 1) for dy in (-1, 0, 1) if (dx, dy) != (0, 0))


def lanes_of(tile, count=1):
    start = (tile + PAD) * LANES
    if not isinstance(start, int):
        start = pl.multiple_of(start, LANES)
    return pl.ds(start, count * LANES)


def rows_sent(dx, depth):
    return {0: pl.ds(0, 8), 1: pl.ds(8 - depth, depth), -1: pl.ds(0, depth)}[dx]


def rows_landed(dx, depth):
    return {0: pl.ds(0, 8), 1: pl.ds(16 - depth, depth), -1: pl.ds(8, depth)}[dx]


def shift_x(value, by):
    return pltpu.roll(value, (-by) % ROWS, 0)


def turn(value, by):
    return pltpu.roll(value, (-by) % LANES, 1)


class Tiles:
    def __init__(self):
        self.known = {}

    def get(self, name, tile, make):
        key = (name, tile)
        if key not in self.known:
            self.known[key] = make()
        return self.known[key]


def flat_shift(memo, name, of, lane, tile, by):
    whole, part = divmod(by, LANES)
    first = memo.get(("turn", name, part), tile + whole, lambda: turn(of(tile + whole), part))
    if part == 0:
        return first
    second = memo.get(("turn", name, part), tile + whole + 1, lambda: turn(of(tile + whole + 1), part))
    return jnp.where(lane < LANES - part, first, second)


def unit_window(memo, of, lane, start, low, high):
    tile, part = divmod(start, LANES)
    if part + low >= LANES:
        tile, part, low, high = tile + 1, part - LANES, low, high
    first = memo.get("turn", (tile, part % LANES), lambda: turn(of(tile), part % LANES))
    if part + high <= LANES:
        return first
    second = memo.get("turn", (tile + 1, part % LANES), lambda: turn(of(tile + 1), part % LANES))
    return jnp.where(lane < LANES - part, first, second)


def to_planes(ref, rows, slots, base, store):
    memo = Tiles()
    lane = lax.broadcasted_iota(jnp.int32, (8, LANES), 1)

    def of(tile):
        return memo.get("load", tile, lambda: ref[rows, lanes_of(base + tile)])

    for slot in slots:
        parts = []
        for c in range(3):
            near = (slot - STEPS) * PLANES + c * THICK
            far = near + HALVES * PLANES - THICK
            parts.append(
                jnp.where(
                    lane < THICK,
                    unit_window(memo, of, lane, near, 0, THICK),
                    unit_window(memo, of, lane, far, THICK, 2 * THICK),
                )
            )
        store(slot, parts)


def from_planes(planes, dst, tiles):
    lane = lax.broadcasted_iota(jnp.int32, (8, LANES), 1)
    for q in tiles:
        out = None
        for n in range(q * LANES // THICK, (q * LANES + LANES - 1) // THICK + 1):
            cell, c = divmod(n, 3)
            far = cell >= HALVES
            slot = cell + STEPS - (HALVES if far else 0)
            value = turn(planes[slot, c, 0:8], q * LANES - n * THICK + (THICK if far else 0))
            out = value if out is None else jnp.where(lane < n * THICK - q * LANES, out, value)
        dst[:, pl.ds(q * LANES, LANES)] = out


def slopes(src, level, slot, sz, sx, ex, ez, lap, rows):
    lane = lax.broadcasted_iota(jnp.int32, (ROWS, LANES), 1)
    keep_up = jnp.where((lane == THICK - 1) | (lane >= 2 * THICK - 1), 0.0, 1.0)
    keep_down = jnp.where((lane == 0) | (lane == THICK), 0.0, 1.0)
    lap_x, lap_z, mixed = [], [], []
    for c in range(3):
        u = src[slot, c]
        up, down = turn(u, 1) * keep_up, turn(u, -1) * keep_down
        right, left = shift_x(u, 1)[:rows], shift_x(u, -1)[:rows]
        slope_z = (up - down) * 0.25
        lap_z.append((up + down)[:rows])
        lap_x.append(right + left)
        if c < 2:
            sx[level, slot, c, 0:rows] = (right - left) * 0.25
        if c > 0:
            sz[level, slot, c - 1, 0:rows] = slope_z[:rows]
        if c != 1:
            mixed.append((shift_x(slope_z, 1) - shift_x(slope_z, -1))[:rows])
        lap[level, slot, c, 0:rows] = lap_x[c] + lap_z[c]
    ex[level, slot, 0:rows] = lap_x[0] + mixed[1]
    ez[level, slot, 0:rows] = lap_z[2] + mixed[0]


def advance_slot(src, old, dst, level, slot, sz, sx, ex, ez, lap, stiff, pushed, rows):
    bulk, shear, light = (stiff[slot, n, 0:rows] for n in range(3))
    centre = [src[slot, c, 0:rows] for c in range(3)]
    lap_y = [src[slot + 1, c, 0:rows] + src[slot - 1, c, 0:rows] for c in range(3)]

    def along(ref, c):
        return ref[level, slot + 1, c, 0:rows] - ref[level, slot - 1, c, 0:rows]

    grad = (
        ex[level, slot, 0:rows] + along(sx, 1),
        lap_y[1] + (along(sx, 0) + along(sz, 1)),
        ez[level, slot, 0:rows] + along(sz, 0),
    )
    for c in range(3):
        twice = centre[c] + centre[c]
        total = lap[level, slot, c, 0:rows] + lap_y[c] - 6.0 * centre[c]
        acc = bulk * (grad[c] - twice) + shear * total
        if c == 2:
            acc = acc + light * pushed
        dst[slot, c, 0:rows] = twice - old[slot, c, 0:rows] + acc
    return acc


def water_block(src, old, dst, mod, ghost, dst_pad, base, tiles, last):
    memo = Tiles()
    lane = lax.broadcasted_iota(jnp.int32, (ROWS, LANES), 1)
    rows = 8 if last else ROWS

    def at(ref, j):
        return ref[:, lanes_of(base + j)]

    def u(j):
        return memo.get("u", j, lambda: at(src, j))

    for j in tiles:
        below = flat_shift(memo, "u", u, lane, j, 1)
        above = flat_shift(memo, "u", u, lane, j, -1)
        offset = (j * LANES) % PLANES
        top = (-offset) % PLANES
        floor = PLANES - 1 - offset
        if top < LANES:
            above = jnp.where(lane == top, 0.0, above)
        if 0 <= floor < LANES:
            below = jnp.where(lane == floor, u(j) - ghost(j), below)
        total = (shift_x(u(j), 1) + shift_x(u(j), -1)) + (below + above)
        total = total + (flat_shift(memo, "u", u, lane, j, PLANES) + flat_shift(memo, "u", u, lane, j, -PLANES))
        total = (total - 6.0 * u(j))[:rows]
        centre = u(j)[:rows]
        new = (centre + centre) - at(old, j)[:rows] + (H2 * at(mod, j)[:rows]) * total
        if last:
            dst[:, pl.ds(dst_pad + j * LANES, LANES)] = new
        else:
            dst[:, lanes_of(base + j)] = new


def top_slopes(src, c, g, at, sz, sx, ex, lap, rows):
    lane = lax.broadcasted_iota(jnp.int32, (ROWS, LANES), 1)
    u = src[c, :, at(g)]
    up, down = turn(u, 1), jnp.where(lane % 16 == 0, 0.0, turn(u, -1))
    right, left = shift_x(u, 1)[:rows], shift_x(u, -1)[:rows]
    slope = (up - down) * 0.25
    sz[c, 0:rows, at(g)] = slope[:rows]
    sx[c, 0:rows, at(g)] = (right - left) * 0.25
    lap_x, lap_z = right + left, (up + down)[:rows]
    lap[c, 0:rows, at(g)] = lap_x + lap_z
    mixed = (shift_x(slope, 1) - shift_x(slope, -1))[:rows]
    ex[c, 0:rows, at(g)] = mixed
    return lap_x, lap_z


def top_update(memo, src, old, dst, g, at, sz, sx, ex, self_terms, lap, stiff, pushed, rows):
    lane = lax.broadcasted_iota(jnp.int32, (rows, LANES), 1)

    def along(name, ref, c, by):
        return flat_shift(memo, (name, c), lambda n: ref[c, 0:rows, at(n)], lane, g, by)

    def cross(name, ref, c):
        return along(name, ref, c, 16) - along(name, ref, c, -16)

    bulk, shear, light = (stiff[n, 0:rows, at(g)] for n in range(3))
    acc = None
    for c in range(3):
        if dst is None and c < 2:
            continue
        u = src[c, 0:rows, at(g)]
        lap_y = along("u", src, c, 16) + along("u", src, c, -16)
        if c == 0:
            grad = self_terms[0, 0:rows, at(g)] + (cross("sx", sx, 1) + ex[2, 0:rows, at(g)])
        elif c == 1:
            grad = lap_y + (cross("sx", sx, 0) + cross("sz", sz, 2))
        else:
            grad = self_terms[1, 0:rows, at(g)] + (ex[0, 0:rows, at(g)] + cross("sz", sz, 1))
        twice = u + u
        total = lap[c, 0:rows, at(g)] + lap_y - 6.0 * u
        acc = bulk * (grad - twice) + shear * total
        if c == 2:
            acc = acc + light * pushed
        if dst is not None:
            dst[c, 0:rows, at(g)] = twice - old[c, 0:rows, at(g)] + acc
    return acc


def floor_lane(tile):
    if tile % PERIOD == 0:
        return None
    return (tile - 1) // PERIOD, 16 * ((tile - 1) % PERIOD) + 15


def exact_dot(a, b):
    return jnp.dot(a, b, precision=lax.Precision.HIGHEST, preferred_element_type=jnp.float32)


def kernel(
    sizes, own_tiles, cur_hbm, prev_hbm, mat_hbm, prior_hbm, fields_ref, floor_ref,
    cur, prev, mat, p1, p2, p3, d0, d1, d2, d3, d4, before, stiff, sz, sx, ex, ez, lap,
    prior, deep, packed, arrived, spread, crown, samples, t0, t1, t2, t3, told, tstiff, tsz, tsx, tex, tself, tlap,
    load_sem, send_sem, recv_sem, deep_send, deep_recv, trace_send, trace_recv, crown_send, crown_recv,
):
    half, gx, gy = lax.axis_index("half"), lax.axis_index("gx"), lax.axis_index("gy")
    n_x, n_y = sizes
    wet = half == 0
    groups = own_tiles // PERIOD

    def exists(dx, dy):
        x, y = gx + dx, gy + dy
        return (x >= 0) & (x < n_x) & (y >= 0) & (y < n_y)

    loads = [
        pltpu.make_async_copy(src.at[0], dst.at[0:8, lanes_of(0, own_tiles)], load_sem.at[n])
        for n, (src, dst) in enumerate(((cur_hbm, cur), (prev_hbm, prev), (mat_hbm, mat)))
    ]
    loads.append(pltpu.make_async_copy(prior_hbm, prior, load_sem.at[3]))
    for copy in loads:
        copy.start()

    barrier = pltpu.get_barrier_semaphore()
    count = jnp.int32(1)
    for dx, dy in DIRS:
        here = exists(dx, dy)
        count = count + 2 * here.astype(jnp.int32)

        @pl.when(here)
        def _(dx=dx, dy=dy):
            for medium in (half, 1 - half):
                there = {"half": medium, "gx": gx + dx, "gy": gy + dy}
                pl.semaphore_signal(barrier, inc=1, device_id=there, device_id_type=MESH)

    pl.semaphore_signal(barrier, inc=1, device_id={"half": 1 - half}, device_id_type=MESH)

    def halo_copies(dx, dy, water):
        short = 1 if water and dx and dy else 0
        out = []
        for n, (ref, reach) in enumerate(((cur, STEPS), (prev, STEPS - 1), (mat, STEPS - 1))):
            depth = reach - short
            width = -(-depth * PLANES // LANES)
            if dy == 0:
                src_lanes = dst_lanes = lanes_of(0, own_tiles)
            elif dy == 1:
                src_lanes, dst_lanes = lanes_of(own_tiles - width, width), lanes_of(-width, width)
            else:
                src_lanes, dst_lanes = lanes_of(0, width), lanes_of(own_tiles, width)
            slot = DIRS.index((dx, dy)) * 3 + n
            out.append(
                pltpu.make_async_remote_copy(
                    src_ref=ref.at[rows_sent(dx, depth), src_lanes],
                    dst_ref=ref.at[rows_landed(dx, depth), dst_lanes],
                    send_sem=send_sem.at[slot],
                    recv_sem=recv_sem.at[slot],
                    device_id={"gx": gx + dx, "gy": gy + dy},
                    device_id_type=MESH,
                )
            )
        return out

    def for_rim(dx, dy, act):
        for water in (True, False):
            @pl.when(wet == water)
            def _(water=water):
                for copy in halo_copies(dx, dy, water):
                    act(copy)

    def deep_lanes(dy, landed):
        if dy == 0:
            return pl.ds(LANES, groups * LANES)
        if landed:
            return pl.ds(0 if dy == 1 else (groups + 1) * LANES, LANES)
        return pl.ds((groups if dy == 1 else 1) * LANES, LANES)

    def deep_copy(dx, dy):
        slot = DIRS.index((dx, dy))
        return pltpu.make_async_remote_copy(
            src_ref=deep.at[rows_sent(dx, STEPS), deep_lanes(dy, False)],
            dst_ref=deep.at[rows_landed(dx, STEPS), deep_lanes(dy, True)],
            send_sem=deep_send.at[slot],
            recv_sem=deep_recv.at[slot],
            device_id={"gx": gx + dx, "gy": gy + dy},
            device_id_type=MESH,
        )

    def crown_copy(dx, dy):
        slot = DIRS.index((dx, dy))
        return pltpu.make_async_remote_copy(
            src_ref=crown.at[:, rows_sent(dx, STEPS), deep_lanes(dy, False)],
            dst_ref=crown.at[:, rows_landed(dx, STEPS), deep_lanes(dy, True)],
            send_sem=crown_send.at[slot],
            recv_sem=crown_recv.at[slot],
            device_id={"half": 1 - half, "gx": gx + dx, "gy": gy + dy},
            device_id_type=MESH,
        )

    def crown_up():
        own = crown.at[:, 0:8, deep_lanes(0, False)]
        return pltpu.make_async_remote_copy(
            src_ref=own, dst_ref=own, send_sem=crown_send.at[len(DIRS)], recv_sem=crown_recv.at[len(DIRS)],
            device_id={"half": 1 - half}, device_id_type=MESH,
        )

    for dx, dy in DIRS:
        @pl.when(jnp.logical_not(exists(-dx, -dy)))
        def _(dx=dx, dy=dy):
            lanes = {0: lanes_of(0, own_tiles), 1: lanes_of(-5, 5), -1: lanes_of(own_tiles, 5)}[dy]
            for ref in (cur, prev, mat):
                ref[rows_landed(dx, STEPS), lanes] = jnp.zeros((8 if dx == 0 else 4, lanes.size), jnp.float32)
            lanes = deep_lanes(dy, True)
            blank = jnp.zeros((8 if dx == 0 else STEPS, lanes.size), jnp.float32)
            deep[rows_landed(dx, STEPS), lanes] = blank
            for c in range(3):
                crown[c, rows_landed(dx, STEPS), lanes] = blank

    for copy in loads:
        copy.wait()
    lane = lax.broadcasted_iota(jnp.int32, (ROWS, LANES), 1)
    lane8 = lane[:8]
    within = lane8 % 16

    @pl.when(wet)
    def _():
        cells = 8 * groups
        row = lax.broadcasted_iota(jnp.int32, (cells, groups * LANES), 0)
        col = lax.broadcasted_iota(jnp.int32, (cells, groups * LANES), 1)
        place = (col == LANES * (row // 8) + 16 * (row % 8) + 15).astype(jnp.float32)
        wave = exact_dot(jnp.concatenate([prior[t] for t in range(STEPS)], 0), place)
        spread[STEPS - 1, 0:8, pl.ds(LANES, groups * LANES)] = wave[8 * (STEPS - 1) :]

        for g in range(groups):
            tile = jnp.zeros((8, LANES), jnp.float32)
            for n, (ref, depth) in enumerate(((cur, STEPS), (prev, STEPS - 1), (mat, STEPS - 1))):
                planes = None
                for j in range(8):
                    value = ref[0:8, lanes_of(g * PERIOD + j + 1)]
                    planes = value if planes is None else jnp.where(lane8 // 16 == j, value, planes)
                tile = tile + turn(jnp.where(within >= 16 - depth, planes, 0.0), 4 * n)
            for t in range(STEPS - 1):
                tile = tile + turn(wave[8 * t : 8 * t + 8, g * LANES : (g + 1) * LANES], 15 - t)
            deep[0:8, pl.ds((g + 1) * LANES, LANES)] = tile

    @pl.when(jnp.logical_not(wet))
    def _():
        for g in range(groups):
            for c in range(3):
                tile = None
                for ref, depth, lead in ((cur, 5, 0), (prev, 4, 5), (mat, 4, 9)):
                    planes = None
                    for j in range(8):
                        q = g * PERIOD + (PLANES * j + THICK * c) // LANES
                        spot = (j + 3 * c) % 8
                        value = ref[0:8, lanes_of(q)]
                        planes = value if planes is None else jnp.where(lane8 // 16 == spot, value, planes)
                    part = jnp.where(within < depth, planes, 0.0)
                    if (THICK * c - lead) % LANES:
                        part = turn(part, THICK * c - lead)
                    tile = part if tile is None else tile + part
                crown[c, 0:8, pl.ds((g + 1) * LANES, LANES)] = tile

    pl.semaphore_wait(barrier, count)


    order = sorted(DIRS, key=lambda d: (d[1] == 0, d[0] != 0))
    for dx, dy in order:
        @pl.when(exists(dx, dy) & wet)
        def _(dx=dx, dy=dy):
            deep_copy(dx, dy).start()

        @pl.when(exists(dx, dy) & jnp.logical_not(wet))
        def _(dx=dx, dy=dy):
            crown_copy(dx, dy).start()

    @pl.when(jnp.logical_not(wet))
    def _():
        crown_up().start()

    for dx, dy in order:
        @pl.when(exists(dx, dy))
        def _(dx=dx, dy=dy):
            for_rim(dx, dy, lambda copy: copy.start())

    def await_rim(dx, dy):
        @pl.when(exists(-dx, -dy))
        def _():
            for_rim(dx, dy, lambda copy: copy.wait_recv())

    levels = (cur, p1, p2, p3)
    olds = (prev, cur, p1, p2)
    width = own_tiles * LANES

    def over_tiles(block, t):
        edge = -(-(STEPS - 1 - t) * PLANES // LANES)
        block(range(-edge, own_tiles + edge))

    def trace_copy(t):
        return pltpu.make_async_remote_copy(
            src_ref=packed.at[t], dst_ref=arrived.at[t], send_sem=trace_send.at[t], recv_sem=trace_recv.at[t],
            device_id={"half": 1 - half}, device_id_type=MESH,
        )

    def dense(value, first):
        cells = 8 * groups
        row = lax.broadcasted_iota(jnp.int32, (LANES, cells), 0)
        col = lax.broadcasted_iota(jnp.int32, (LANES, cells), 1)
        pick = (row == 16 * (col % 8) + first + col // 8).astype(jnp.float32)
        return exact_dot(value, pick)

    @pl.when(wet)
    def _():
        for dx, dy in DIRS:
            @pl.when(exists(-dx, -dy))
            def _(dx=dx, dy=dy):
                deep_copy(dx, dy).wait_recv()

        blocks = range(-1, groups + 1)
        floor_lanes = lane % 16 == 15

        def send_trace(t, tiles):
            for g in blocks:
                samples[t, :, pl.ds((g + 1) * LANES, LANES)] = jnp.where(lane % 16 == 0, turn(tiles[g], 15), 0.0)
            total = None
            for g in blocks:
                tile = turn(jnp.where(floor_lanes, tiles[g], 0.0), 15 - (g + 1))
                total = tile if total is None else total + tile
            packed[t] = total
            trace_copy(t).start()

        def ghost_tile(t, g):
            return spread[t, :, pl.ds((g + 1) * LANES, LANES)]

        now = {g: deep[:, pl.ds((g + 1) * LANES, LANES)] for g in blocks}
        send_trace(0, now)
        then = {g: turn(now[g], -4) for g in blocks}
        speed = {g: turn(now[g], -8) for g in blocks}
        for t in range(STEPS - 1):
            for g in blocks:
                spread[t, :, pl.ds((g + 1) * LANES, LANES)] = turn(now[g], t - 15)
        for t in range(STEPS - 1):
            memo = Tiles()
            later = {}
            inside = {g: now[g] for g in blocks}
            inside[-2] = inside[groups + 1] = jnp.zeros((ROWS, LANES), jnp.float32)

            def of(g, inside=inside):
                return inside[g]

            for g in blocks:
                u = now[g]
                below = jnp.where(floor_lanes, u - ghost_tile(t, g), turn(u, 1))
                total = (shift_x(u, 1) + shift_x(u, -1)) + (below + turn(u, -1))
                total = total + (
                    flat_shift(memo, "u", of, lane, g, 16) + flat_shift(memo, "u", of, lane, g, -16)
                )
                later[g] = (u + u) - then[g] + (H2 * speed[g]) * (total - 6.0 * u)
            then, now = now, later
            send_trace(t + 1, now)

        for dx, dy in DIRS:
            @pl.when(exists(-dx, -dy))
            def _(dx=dx, dy=dy):
                crown_copy(dx, dy).wait_recv()

        crown_up().wait_recv()

        def at(g):
            return pl.ds((g + 2) * LANES, LANES)

        first_lanes = lane % 16 == 0
        for ref in (t0, t1, t2, t3, tsz, tsx):
            for c in range(3):
                for g in (-2, groups + 1):
                    ref[c, :, at(g)] = jnp.zeros((ROWS, LANES), jnp.float32)
        for g in blocks:
            tiles = [crown[c, :, pl.ds((g + 1) * LANES, LANES)] for c in range(3)]
            light = H2 * turn(tiles[2], 9)
            tstiff[0, :, at(g)] = light * turn(tiles[0], 9)
            tstiff[1, :, at(g)] = light * turn(tiles[1], 9)
            tstiff[2, :, at(g)] = light
            for c in range(3):
                t0[c, :, at(g)] = tiles[c]
                told[c, :, at(g)] = turn(tiles[c], 5)

        tops, befores = (t0, t1, t2, t3, None), (told, t0, t1, t2)
        for t in range(STEPS):
            last = t == STEPS - 1
            rows = 8 if last else ROWS
            for g in blocks:
                terms = [top_slopes(tops[t], c, g, at, tsz, tsx, tex, tlap, rows) for c in range(3)]
                tself[0, 0:rows, at(g)] = terms[0][0]
                tself[1, 0:rows, at(g)] = terms[2][1]
            total = None
            memo = Tiles()
            for g in range(groups) if last else blocks:
                source = samples[t, 0:rows, pl.ds((g + 1) * LANES, LANES)]
                acc = top_update(
                    memo, tops[t], befores[t], tops[t + 1], g, at, tsz, tsx, tex, tself, tlap, tstiff, source, rows
                )
                if 0 <= g < groups:
                    tile = turn(jnp.where(within == 0, acc[:8], 0.0), -g)
                    total = tile if total is None else total + tile
            floor_ref[0, t] = (RELAXATION / H2) * dense(total, 0) + (1.0 - RELAXATION) * prior[t]
            trace_copy(t).wait_send()

        for dx, dy in DIRS:
            await_rim(dx, dy)

        for t in range(STEPS):
            src, old = levels[t], olds[t]
            last = t == STEPS - 1

            def block(tiles, t=t, src=src, old=old, last=last):
                def ghost(j):
                    return ghost_tile(t, (j - 1) // PERIOD)

                dst = fields_ref.at[0] if last else levels[t + 1]
                water_block(src, old, dst, mat, ghost, 0, 0, tiles, last)

            over_tiles(block, t)

    @pl.when(jnp.logical_not(wet))
    def _():
        def convert(rows, slots, base=0, shift=0):
            def put(ref):
                def store(slot, parts):
                    for c in range(3):
                        ref[slot + shift, c, rows] = parts[c]
                return store

            def put_stiff(slot, parts):
                light = H2 * parts[2]
                stiff[slot + shift, 0, rows] = light * parts[0]
                stiff[slot + shift, 1, rows] = light * parts[1]
                stiff[slot + shift, 2, rows] = light

            inner = [slot for slot in slots if 0 < slot < SLOTS - 1]
            to_planes(cur, rows, slots, base, put(d0))
            to_planes(prev, rows, inner, base, put(before))
            to_planes(mat, rows, inner, base, put_stiff)

        def convert_inner(rows):
            @pl.loop(0, HALVES // 8)
            def _(n):
                convert(rows, range(STEPS, STEPS + 8), n * PERIOD, n * 8)

        upper, lower = pl.ds(0, 8), pl.ds(8, 8)
        convert_inner(upper)
        for dx, dy in DIRS:
            if dy == 0:
                await_rim(dx, dy)
        convert_inner(lower)
        for dx, dy in DIRS:
            if dy != 0:
                await_rim(dx, dy)
        for rows in (upper, lower):
            convert(rows, (*range(STEPS), *range(SLOTS - STEPS, SLOTS)))

        displaced = (d0, d1, d2, d3, d4)
        earlier = (before, d0, d1, d2)
        scratch = (sz, sx, ex, ez, lap)
        for t in range(STEPS):
            last = t == STEPS - 1
            rows = 8 if last else ROWS
            src, old, dst = displaced[t], earlier[t], displaced[t + 1]

            for slot in range(t, SLOTS - t):
                slopes(src, t, slot, *scratch, rows)

            trace_copy(t).wait_recv()
            load = arrived[t][:rows]
            lane_out = lane[:rows]

            def pushed(slot, load=load, lane_out=lane_out):
                cell = slot - STEPS
                near = cell % 8 * 16 + 1 + cell // 8
                return jnp.where(
                    lane_out == 0, turn(load, near),
                    jnp.where(lane_out == THICK, turn(load, near + HALVES // 8 - THICK), 0.0),
                )

            for slot in range(t + 1, SLOTS - 1 - t):
                advance_slot(src, old, dst, t, slot, *scratch, stiff, pushed(slot), rows)

        from_planes(d4, fields_ref.at[0], range(own_tiles))
        for t in range(STEPS):
            floor_ref[0, t] = dense(arrived[t, 0:8], 1)
        crown_up().wait_send()

    for dx, dy in DIRS:
        @pl.when(exists(dx, dy))
        def _(dx=dx, dy=dy):
            for_rim(dx, dy, lambda copy: copy.wait_send())

            @pl.when(wet)
            def _():
                deep_copy(dx, dy).wait_send()

            @pl.when(jnp.logical_not(wet))
            def _():
                crown_copy(dx, dy).wait_send()


def deliver(fields_ref, floor_ref, fields_out, floor_out, sem):
    copies = [
        pltpu.make_async_copy(src, dst, sem.at[n])
        for n, (src, dst) in enumerate(((fields_ref, fields_out), (floor_ref, floor_out)))
    ]
    for copy in copies:
        copy.start()
    for copy in copies:
        copy.wait()


def on_device(sizes, current, previous, material, prior):
    own = current.shape[2]
    own_tiles = own // LANES
    groups = own_tiles // PERIOD
    cells = own // PLANES
    field = pltpu.VMEM((ROWS, (own_tiles + 2 * PAD) * LANES), jnp.float32)
    planes = pltpu.VMEM((SLOTS, 3, ROWS, LANES), jnp.float32)

    def per_level(count):
        return pltpu.VMEM((STEPS, SLOTS) + count + (ROWS, LANES), jnp.float32)

    anywhere = pl.BlockSpec(memory_space=pl.ANY)
    near = pl.BlockSpec(memory_space=pltpu.VMEM)
    dma = pltpu.SemaphoreType.DMA
    held = pl.pallas_call(
        functools.partial(kernel, sizes, own_tiles),
        out_shape=(
            pltpu.VMEM(current.shape, jnp.float32),
            pltpu.VMEM((1,) + prior.shape, jnp.float32),
        ),
        in_specs=[anywhere] * 4,
        out_specs=(near, near),
        scratch_shapes=[field] * 6
        + [planes] * 7
        + [per_level((2,)), per_level((2,)), per_level(()), per_level(()), per_level((3,))]
        + [
            pltpu.VMEM(prior.shape, jnp.float32),
            pltpu.VMEM((ROWS, (groups + 2) * LANES), jnp.float32),
            pltpu.VMEM((STEPS, ROWS, LANES), jnp.float32),
            pltpu.VMEM((STEPS, ROWS, LANES), jnp.float32),
            pltpu.VMEM((STEPS, ROWS, (groups + 2) * LANES), jnp.float32),
            pltpu.VMEM((3, ROWS, (groups + 2) * LANES), jnp.float32),
            pltpu.VMEM((STEPS, ROWS, (groups + 2) * LANES), jnp.float32),
            *[pltpu.VMEM((3, ROWS, (groups + 4) * LANES), jnp.float32)] * 11,
            dma((4,)),
            dma((3 * len(DIRS),)),
            dma((3 * len(DIRS),)),
            dma((len(DIRS),)),
            dma((len(DIRS),)),
            dma((STEPS,)),
            dma((STEPS,)),
            dma((len(DIRS) + 1,)),
            dma((len(DIRS) + 1,)),
        ],
        compiler_params=pltpu.CompilerParams(collective_id=0, has_side_effects=True),
    )(current, previous, material, prior)
    return pl.pallas_call(
        deliver,
        out_shape=tuple(jax.ShapeDtypeStruct(x.shape, x.dtype) for x in held),
        in_specs=[near] * 2,
        out_specs=(anywhere, anywhere),
        scratch_shapes=[dma((2,))],
    )(*(pltpu.with_memory_space_constraint(x, pltpu.VMEM) for x in held))


def solution(mesh):
    placed = (
        P("half", "gx", "gy"),
        P("half", "gx", "gy"),
        P("half", "gx", "gy"),
        P(None, "gx", "gy"),
    )
    return jax.shard_map(
        functools.partial(on_device, (mesh.shape["gx"], mesh.shape["gy"])),
        mesh=mesh,
        in_specs=placed,
        out_specs=(P("half", "gx", "gy"), P("half", None, "gx", "gy")),
        check_vma=False,
    )
```
